256 devices in a mesh: seq: 64 (over z, y, core), hid: 4 (over x).
Axes of the slice: x: 4, y: 4, z: 8, core: 2. Of those that a mesh axis runs over, the one named last changes fastest.
Arguments:
- gate_half: bfloat16 [8192, 2048], P('seq', 'hid'), may hold values from -6 to 6
- value_half: bfloat16 [8192, 2048], P('seq', 'hid'), may hold values from -6 to 6
- norm_gain: float32 [2048], P('hid'), may hold values from 0.25 to 1.75
- norm_shift: float32 [2048], P('hid'), may hold values from -0.5 to 0.5
- token_weight: bfloat16 [8192, 8192], P('seq'), may hold values from -0.1875 to 0.1875
- token_bias: float32 [8192], P('seq'), may hold values from 0.5 to 1.5
- grad_output: bfloat16 [8192, 2048], P('seq', 'hid'), may hold values from -6 to 6
Outputs:
- grad_gate: bfloat16 [8192, 2048], P('seq', 'hid')
- grad_value: bfloat16 [8192, 2048], P('seq', 'hid')
- grad_gain: float32 [2048], P('hid')
- grad_shift: float32 [2048], P('hid')
- grad_weight: float32 [8192, 8192], P('seq', 'hid')
- grad_token_bias: float32 [8192], P('seq')
The draws below stay inside these ranges and needn't reach their ends.
All inputs are finite; a program needn't handle non-finite values.
Results may differ from the reference program's by a relative error of at most 0.005.
Values may be sent and summed in bfloat16 or wider, within the bound.
A program may use at most 64 MiB of HBM per device.

```python
import jax
import jax.numpy as jnp
from jax import lax

HIDDEN_SIZE = 2048
TOKENS = 8192


def with_spikes(result, rng, source, target, parts, factor):
    owner, partner = [(jnp.arange(result.shape[axis_at]) // (result.shape[axis_at] // parts)).reshape([-1 if axis == axis_at else 1 for axis in range(result.ndim)]) for axis_at in (source, target)]
    chosen = jax.random.permutation(rng, parts)[partner]
    strong = (owner == chosen) | (owner == (partner + parts // 2) % parts)
    return jnp.where(strong, factor * result, result)


def block_scale(stream_key, dims, cuts, smallest, largest):
    loudness, own = 1.0, jax.random.fold_in(stream_key, 6)
    for position, blocks in cuts:
        steps = jnp.exp(jax.random.uniform(jax.random.fold_in(own, position), (blocks,), jnp.float32, smallest / len(cuts), largest / len(cuts)))
        loudness = loudness * jnp.repeat(steps, dims[position] // blocks).reshape([-1 if axis == position else 1 for axis in range(len(dims))])
    return loudness


def bell_draw(rng, extent, width, reach, cuts=(), kind=jnp.bfloat16):
    result = width * jax.random.normal(rng, extent, jnp.float32)
    if cuts:
        result = result * block_scale(rng, extent, cuts, -0.22, 0.18)
    return jnp.clip(result, -reach, reach).astype(kind)


def bell_draw_with(rng, extent, width, bound, split, heavy, held_as=jnp.bfloat16):
    array = width * jax.random.normal(rng, extent, jnp.float32)
    if split:
        array = array * block_scale(rng, extent, split, -0.22, 0.18)
    return jnp.clip(with_spikes(array, jax.random.fold_in(rng, 3), *heavy), -bound, bound).astype(held_as)


def setup_inputs(seed: int = 0) -> dict:
    arg_keys = jax.random.split(jax.random.key(seed), 8)
    gate_half = bell_draw(arg_keys[0], (TOKENS, HIDDEN_SIZE), 1.0, 6.0, ((0, 64), (1, 4)))
    value_half = bell_draw(arg_keys[1], (TOKENS, HIDDEN_SIZE), 1.0, 6.0, ((0, 64), (1, 4)))
    norm_gain = jnp.clip(1.0 + 0.15 * jax.random.normal(arg_keys[2], (HIDDEN_SIZE,), jnp.float32), 0.25, 1.75)
    norm_shift = jnp.clip(jax.random.uniform(arg_keys[3], (HIDDEN_SIZE,), jnp.float32, -0.5, 0.5) * block_scale(arg_keys[3], (HIDDEN_SIZE,), ((0, 4),), -0.4, 0.0), -0.5, 0.5)
    token_weight = bell_draw_with(arg_keys[4], (TOKENS, TOKENS), TOKENS ** -0.5, 0.1875, ((0, 64),), (0, 1, 64, 4.0))
    token_bias = jnp.clip(0.5 + 1.0 * jax.random.uniform(arg_keys[5], (TOKENS,), jnp.float32) ** block_scale(arg_keys[5], (TOKENS,), ((0, 64),), -0.2, 0.2), 0.5, 1.5)
    grad_output = bell_draw(arg_keys[6], (TOKENS, HIDDEN_SIZE), 1.0, 6.0, ((0, 64), (1, 4)))
    return {"gate_half": gate_half, "value_half": value_half, "norm_gain": norm_gain, "norm_shift": norm_shift, "token_weight": token_weight, "token_bias": token_bias, "grad_output": grad_output}


def reference(gate_half, value_half, norm_gain, norm_shift, token_weight, token_bias, grad_output):
    second = value_half.astype(jnp.float32)
    row_mean = lax.optimization_barrier(jnp.sum(second, axis=1, keepdims=True)) / HIDDEN_SIZE
    row_var = lax.optimization_barrier(jnp.sum(second * second, axis=1, keepdims=True)) / HIDDEN_SIZE - row_mean * row_mean
    inv_std = lax.rsqrt(row_var + 1e-05)
    centred = (second - row_mean) * inv_std
    normed = (centred * norm_gain + norm_shift).astype(jnp.bfloat16)
    lower_weight = jnp.tril(token_weight)
    spatial = jnp.dot(lower_weight, normed, preferred_element_type=jnp.float32) + token_bias[:, None]
    upstream = grad_output.astype(jnp.float32)
    grad_gate = (upstream * spatial).astype(jnp.bfloat16)
    grad_mix = (upstream * gate_half.astype(jnp.float32)).astype(jnp.bfloat16)
    grad_weight = jnp.tril(jnp.dot(grad_mix, normed.T, preferred_element_type=jnp.float32))
    grad_token_bias = lax.optimization_barrier(jnp.sum(grad_mix.astype(jnp.float32), axis=1))
    grad_normed = jnp.dot(lower_weight.T, grad_mix, preferred_element_type=jnp.float32)
    grad_gain = lax.optimization_barrier(jnp.sum(grad_normed * centred, axis=0))
    grad_shift = lax.optimization_barrier(jnp.sum(grad_normed, axis=0))
    grad_centred = grad_normed * norm_gain
    first_mean = lax.optimization_barrier(jnp.sum(grad_centred, axis=1, keepdims=True)) / HIDDEN_SIZE
    second_mean = lax.optimization_barrier(jnp.sum(grad_centred * centred, axis=1, keepdims=True)) / HIDDEN_SIZE
    grad_value = (inv_std * (grad_centred - first_mean - centred * second_mean)).astype(jnp.bfloat16)
    return (grad_gate, grad_value, grad_gain, grad_shift, grad_weight, grad_token_bias)
```

```python
import functools

import jax
import jax.numpy as jnp
from jax import lax
from jax.experimental import pallas as pl
from jax.experimental.pallas import tpu as pltpu
from jax.sharding import PartitionSpec as P

MESH = pl.DeviceIdType.MESH
F32 = jnp.float32
BF16 = jnp.bfloat16
T = 128
R = 8
Z = 8
X = 4


def dot(a, b, ca, cb):
    return lax.dot_general(a, b, (((ca,), (cb,)), ((), ())), preferred_element_type=F32)


def kernel(
    hidden,
    gate, value, gain, shift, w, tbias, go,
    gg_out, gv_out, gs_out, gw_out, tb_out,
    g_all, n_all, wt, s_acc, s_send, s_recv, gn_own, gn_send, gn_recv, gw_send, gwx_recv, gwr, gwf,
    stat1, stat2, red1, red2, cen, rows,
    g_ss, g_rs, w_ss, w_rs, n_ss, n_rs, s_ss, s_rs, gn_ss, gn_rs, gx_ss, gx_rs, gf_ss, gf_rs,
    st_ss, st_rs, sp_ss, sp_rs, ra_ss, ra_rs, rb_ss, rb_rs,
):
    s = lax.axis_index("seq")
    x = lax.axis_index("hid")
    z = s // R
    r = s % R

    def rcopy(src, dst, ss, rs, ds, dx):
        return pltpu.make_async_remote_copy(
            src_ref=src, dst_ref=dst, send_sem=ss, recv_sem=rs,
            device_id=(ds, dx), device_id_type=MESH,
        )

    def plane(d):
        q = (r + d) % R
        return q, z * R + q

    barrier = pltpu.get_barrier_semaphore()
    for d in range(1, R):
        q, dev = plane(d)
        pl.semaphore_signal(barrier, inc=1, device_id=(dev, x), device_id_type=MESH)
    for d in range(1, Z):
        pl.semaphore_signal(
            barrier, inc=1, device_id=(((z + d) % Z) * R + r, x), device_id_type=MESH
        )
    for d in range(1, X):
        pl.semaphore_signal(barrier, inc=1, device_id=(s, (x + d) % X), device_id_type=MESH)

    v = value[...].astype(F32)
    gm = (go[...].astype(F32) * gate[...].astype(F32)).astype(BF16)
    g_all[r] = gm
    lane = lax.broadcasted_iota(jnp.int32, (T, T), 1)

    def as_rows(cols):
        m = jnp.zeros((T, T), F32)
        for i, col in enumerate(cols):
            m = jnp.where(lane == i, col, m)
        return m.T[:8]

    stat1[x] = as_rows((
        jnp.sum(v, axis=1, keepdims=True),
        jnp.sum(v * v, axis=1, keepdims=True),
        jnp.sum(gm.astype(F32), axis=1, keepdims=True),
    ))
    pl.semaphore_wait(barrier, (R - 1) + (Z - 1) + (X - 1))

    def x_send(buf, ss, rs):
        for d in range(1, X):
            t = (x + d) % X
            rcopy(buf.at[x], buf.at[x], ss.at[d], rs.at[x], s, t).start()

    def x_wait(buf, ss, rs):
        for d in range(1, X):
            t = (x + d) % X
            c = rcopy(buf.at[x], buf.at[t], ss.at[d], rs.at[t], s, t)
            c.wait_recv()
            c.wait_send()

    x_send(stat1, st_ss, st_rs)
    for d in range(1, R):
        q, dev = plane(d)
        rcopy(g_all.at[r], g_all.at[r], g_ss.at[d], g_rs.at[r], dev, x).start()

    def w_send(k, carry):
        zz = z - k
        for d in range(1, R):
            q, dev = plane(d)
            cols = pl.ds(pl.multiple_of((zz * R + q) * T, T), T)
            rcopy(w.at[:, cols], wt.at[zz, r], w_ss.at[zz, d], w_rs.at[zz, r], dev, x).start()
        return carry

    lax.fori_loop(0, z + 1, w_send, 0)

    x_wait(stat1, st_ss, st_rs)
    tot = stat1[0] + stat1[1] + stat1[2] + stat1[3]
    tb_out[...] = tot[2:3]
    colm = jnp.concatenate([tot[:3], tbias[...], jnp.zeros((T - 4, T), F32)], axis=0).T
    mean = colm[:, 0:1] / hidden
    var = colm[:, 1:2] / hidden - mean * mean
    inv = lax.rsqrt(var + 1e-05)
    centred = (v - mean) * inv
    cen[...] = centred
    rows[0] = jnp.broadcast_to(inv, (T, T))
    rows[1] = jnp.broadcast_to(colm[:, 3:4], (T, T))
    n_all[z] = (centred * gain[...] + shift[...]).astype(BF16)

    def n_send(k, carry):
        zz = Z - 1 - k
        rcopy(n_all.at[z], n_all.at[z], n_ss.at[zz], n_rs.at[z], zz * R + r, x).start()
        return carry

    lax.fori_loop(0, Z - 1 - z, n_send, 0)

    for d in range(1, R):
        q, dev = plane(d)
        rcopy(g_all.at[q], g_all.at[q], g_ss.at[d], g_rs.at[q], dev, x).wait_recv()

    def step(k, carry):
        zz = z - k
        for d in range(1, R):
            q, dev = plane(d)
            rcopy(wt.at[zz, q], wt.at[zz, q], w_ss.at[zz, d], w_rs.at[zz, q], dev, x).wait_recv()
        wt[zz, r] = w[:, pl.ds(pl.multiple_of((zz * R + r) * T, T), T)]

        @pl.when(k == 0)
        def _():
            row = lax.broadcasted_iota(jnp.int32, (T, T), 0)
            own = wt[zz, r].astype(F32)
            wt[zz, r] = jnp.where(row >= lane, own, 0.0).astype(BF16)

            def clear(q, c):
                wt[zz, q] = jnp.zeros((T, T), BF16)
                return c

            lax.fori_loop(0, r, clear, 0)

        wz = wt[zz].reshape(R * T, T)
        gz = g_all[...].reshape(R * T, -1)
        gn = dot(wz, gz, 0, 0)

        @pl.when(k == 0)
        def _():
            gn_own[...] = gn

        @pl.when(k > 0)
        def _():
            gn_send[zz] = gn.astype(BF16)
            rcopy(
                gn_send.at[zz], gn_recv.at[z], gn_ss.at[zz], gn_rs.at[z], zz * R + r, x
            ).start()
            rcopy(
                n_all.at[zz], n_all.at[zz], n_ss.at[zz], n_rs.at[zz], zz * R + r, x
            ).wait_recv()

        nz = n_all[zz]
        gw_send[zz] = dot(gz, nz, 1, 1).astype(BF16)
        t = zz // 2

        @pl.when(t != x)
        def _():
            rcopy(
                gw_send.at[zz], gwx_recv.at[zz % 2, x], gx_ss.at[zz], gx_rs.at[zz % 2, x], s, t
            ).start()

        sp = dot(wz, nz, 1, 0)

        @pl.when(k == 0)
        def _():
            s_acc[...] = sp

        @pl.when(k > 0)
        def _():
            s_acc[...] += sp

        return carry

    lax.fori_loop(0, z + 1, step, 0)

    for d in range(1, R):
        q, dev = plane(d)
        s_send[q] = s_acc[pl.ds(pl.multiple_of(q * T, T), T), :].astype(BF16)
        rcopy(s_send.at[q], s_recv.at[r], s_ss.at[d], s_rs.at[r], dev, x).start()

    for b in range(2):
        zb = 2 * x + b

        @pl.when(zb <= z)
        def _():
            acc = gw_send[zb].astype(F32)
            for d in range(1, X):
                t = (x + d) % X
                rcopy(
                    gw_send.at[zb], gwx_recv.at[b, t], gx_ss.at[zb], gx_rs.at[b, t], s, t
                ).wait_recv()
                acc = acc + gwx_recv[b, t].astype(F32)
            gwr[b] = acc.astype(BF16).reshape(R, T, T)
            for d in range(1, R):
                q, dev = plane(d)
                rcopy(
                    gwr.at[b, q], gwf.at[b, r], gf_ss.at[b, d], gf_rs.at[b, r], dev, x
                ).start()
            gwf[b, r] = gwr[b, r]

        @pl.when(zb > z)
        def _():
            gwf[b] = jnp.zeros((R, T, T), BF16)

    acc = s_acc[pl.ds(pl.multiple_of(r * T, T), T), :]
    for d in range(1, R):
        q, dev = plane(d)
        rcopy(s_send.at[q], s_recv.at[q], s_ss.at[d], s_rs.at[q], dev, x).wait_recv()
        acc = acc + s_recv[q].astype(F32)
    gg_out[...] = (go[...].astype(F32) * (acc + rows[1][:, 0:1])).astype(BF16)

    def gn_wait(k, carry):
        zz = z + 1 + k
        rcopy(
            gn_send.at[zz], gn_recv.at[zz], gn_ss.at[zz], gn_rs.at[zz], zz * R + r, x
        ).wait_recv()
        gn_own[...] += gn_recv[zz].astype(F32)
        return carry

    lax.fori_loop(0, Z - 1 - z, gn_wait, 0)
    gn = gn_own[...]
    centred = cen[...]
    gc = gn * gain[...]
    stat2[x] = as_rows((
        jnp.sum(gc, axis=1, keepdims=True),
        jnp.sum(gc * centred, axis=1, keepdims=True),
    ))
    x_send(stat2, sp_ss, sp_rs)
    red1[r] = jnp.concatenate([
        jnp.sum(gn * centred, axis=0, keepdims=True),
        jnp.sum(gn, axis=0, keepdims=True),
        jnp.zeros((6, gn.shape[1]), F32),
    ], axis=0)
    for d in range(1, R):
        q, dev = plane(d)
        rcopy(red1.at[r], red1.at[r], ra_ss.at[d], ra_rs.at[r], dev, x).start()
    x_wait(stat2, sp_ss, sp_rs)
    tot = stat2[0] + stat2[1] + stat2[2] + stat2[3]
    colm = jnp.concatenate([tot, jnp.zeros((T - 8, T), F32)], axis=0).T
    gv_out[...] = (
        rows[0][:, 0:1] * (gc - colm[:, 0:1] / hidden - centred * (colm[:, 1:2] / hidden))
    ).astype(BF16)
    for d in range(1, R):
        q, dev = plane(d)
        c = rcopy(red1.at[r], red1.at[q], ra_ss.at[d], ra_rs.at[q], dev, x)
        c.wait_recv()
        c.wait_send()
    tot = red1[0]
    for q in range(1, R):
        tot = tot + red1[q]
    red2[z] = tot
    for d in range(1, Z):
        zz = (z + d) % Z
        rcopy(red2.at[z], red2.at[z], rb_ss.at[d], rb_rs.at[z], zz * R + r, x).start()

    for b in range(2):
        zb = 2 * x + b

        @pl.when(zb <= z)
        def _():
            for d in range(1, R):
                q, dev = plane(d)
                c = rcopy(gwr.at[b, q], gwf.at[b, q], gf_ss.at[b, d], gf_rs.at[b, q], dev, x)
                c.wait_recv()
                c.wait_send()

        for q in range(R):
            gw_out[:, (b * R + q) * T : (b * R + q + 1) * T] = gwf[b, q]

    for d in range(1, Z):
        zz = (z + d) % Z
        c = rcopy(red2.at[z], red2.at[zz], rb_ss.at[d], rb_rs.at[zz], zz * R + r, x)
        c.wait_recv()
        c.wait_send()
    tot = red2[0]
    for q in range(1, Z):
        tot = tot + red2[q]
    gs_out[...] = tot

    for d in range(1, R):
        q, dev = plane(d)
        rcopy(g_all.at[r], g_all.at[r], g_ss.at[d], g_rs.at[r], dev, x).wait_send()
        rcopy(s_send.at[q], s_recv.at[r], s_ss.at[d], s_rs.at[r], dev, x).wait_send()

    def drain_w(zz, carry):
        for d in range(1, R):
            q, dev = plane(d)
            rcopy(wt.at[zz, q], wt.at[zz, r], w_ss.at[zz, d], w_rs.at[zz, r], dev, x).wait_send()

        @pl.when(zz // 2 != x)
        def _():
            rcopy(
                gw_send.at[zz], gwx_recv.at[zz % 2, x], gx_ss.at[zz], gx_rs.at[zz % 2, x],
                s, zz // 2,
            ).wait_send()

        return carry

    lax.fori_loop(0, z + 1, drain_w, 0)

    def drain_gn(zz, carry):
        rcopy(
            gn_send.at[zz], gn_recv.at[z], gn_ss.at[zz], gn_rs.at[z], zz * R + r, x
        ).wait_send()
        return carry

    lax.fori_loop(0, z, drain_gn, 0)

    def drain_n(zz, carry):
        rcopy(n_all.at[z], n_all.at[z], n_ss.at[zz], n_rs.at[z], zz * R + r, x).wait_send()
        return carry

    lax.fori_loop(z + 1, Z, drain_n, 0)


def per_device(gate_half, value_half, norm_gain, norm_shift, token_weight, token_bias, grad_output):
    rows, chans = gate_half.shape
    cols = token_weight.shape[1]
    width = cols // X
    dma = pltpu.SemaphoreType.DMA
    vmem = pl.BlockSpec(memory_space=pltpu.VMEM)
    gg, gv, gs, gw, tb = pl.pallas_call(
        functools.partial(kernel, chans * X),
        out_shape=(
            jax.ShapeDtypeStruct((rows, chans), BF16),
            jax.ShapeDtypeStruct((rows, chans), BF16),
            jax.ShapeDtypeStruct((8, chans), F32),
            jax.ShapeDtypeStruct((rows, width), BF16),
            jax.ShapeDtypeStruct((1, rows), F32),
        ),
        in_specs=[vmem] * 7,
        out_specs=(vmem,) * 5,
        scratch_shapes=[
            pltpu.VMEM((R, T, chans), BF16),
            pltpu.VMEM((Z, T, chans), BF16),
            pltpu.VMEM((Z, R, T, T), BF16),
            pltpu.VMEM((R * T, chans), F32),
            pltpu.VMEM((R, T, chans), BF16),
            pltpu.VMEM((R, T, chans), BF16),
            pltpu.VMEM((T, chans), F32),
            pltpu.VMEM((Z, T, chans), BF16),
            pltpu.VMEM((Z, T, chans), BF16),
            pltpu.VMEM((Z, R * T, T), BF16),
            pltpu.VMEM((2, X, R * T, T), BF16),
            pltpu.VMEM((2, R, T, T), BF16),
            pltpu.VMEM((2, R, T, T), BF16),
            pltpu.VMEM((X, 8, T), F32),
            pltpu.VMEM((X, 8, T), F32),
            pltpu.VMEM((R, 8, chans), F32),
            pltpu.VMEM((Z, 8, chans), F32),
            pltpu.VMEM((T, chans), F32),
            pltpu.VMEM((2, T, T), F32),
            dma((R,)), dma((R,)),
            dma((Z, R)), dma((Z, R)),
            dma((Z,)), dma((Z,)),
            dma((R,)), dma((R,)),
            dma((Z,)), dma((Z,)),
            dma((Z,)), dma((2, X)),
            dma((2, R)), dma((2, R)),
            dma((X,)), dma((X,)),
            dma((X,)), dma((X,)),
            dma((R,)), dma((R,)),
            dma((Z,)), dma((Z,)),
        ],
        compiler_params=pltpu.CompilerParams(
            collective_id=0, has_side_effects=True, vmem_limit_bytes=48 * 1024 * 1024
        ),
    )(
        gate_half, value_half, norm_gain[None], norm_shift[None], token_weight, token_bias[None],
        grad_output,
    )
    row = lax.axis_index("seq") * rows + lax.iota(jnp.int32, rows)[:, None]
    col = lax.axis_index("hid") * width + lax.iota(jnp.int32, width)[None, :]
    grad_weight = jnp.where(col <= row, gw.astype(F32), 0.0)
    return gg, gv, gs[0], gs[1], grad_weight, tb[0]


def solution(mesh):
    placed = (
        P("seq", "hid"),
        P("seq", "hid"),
        P("hid"),
        P("hid"),
        P("seq", None),
        P("seq"),
        P("seq", "hid"),
    )
    return jax.shard_map(
        per_device,
        mesh=mesh,
        in_specs=placed,
        out_specs=(P("seq", "hid"), P("seq", "hid"), P("hid"), P("hid"), P("seq", "hid"), P("seq")),
        check_vma=False,
    )
```

```python
import contextlib
import functools

import jax
import jax.numpy as jnp
from jax import lax
from jax.experimental import pallas as pl
from jax.experimental.pallas import tpu as pltpu
from jax.sharding import PartitionSpec as P

MESH = pl.DeviceIdType.MESH
F32 = jnp.float32
BF16 = jnp.bfloat16
T = 128
R = 8
Z = 8
X = 4
Y = 4


def at(name):
    return contextlib.nullcontext()


def dot(a, b, ca, cb):
    return lax.dot_general(a, b, (((ca,), (cb,)), ((), ())), preferred_element_type=F32)


def kernel(
    hidden,
    gate_h, value_h, gain_h, shift_h, w_h, tbias_h, go_h,
    gg_out, gv_out, gs_out, gw_out, tb_out,
    g_all, n_all, wt, s_acc, s_sib, s_send, s_recv, gn_own, gn_send, gn_recv,
    gw_send, gwo, gwx, gwr, gwf,
    stat1, stat2, red1, red2, cen, rows,
    gate, value, gain, shift, w, tbias, go, in_sem,
    gg, gv, gs, gw, tb, out_sem,
    g_ss, g_rs, w_ss, w_rs, n_ss, n_rs, sb_ss, sb_rs, s_ss, s_rs, gn_ss, gn_rs,
    go_ss, go_rs, gx_ss, gx_rs, gf_ss, gf_rs,
    st_ss, st_rs, sp_ss, sp_rs, ra_ss, ra_rs, rb_ss, rb_rs,
):
    s = lax.axis_index("seq")
    x = lax.axis_index("hid")
    z = s // R
    r = s % R
    y = r // 2
    c = r % 2
    sib = z * R + y * 2 + (1 - c)
    H = R * T // 2

    def rcopy(src, dst, ss, rs, ds, dx):
        return pltpu.make_async_remote_copy(
            src_ref=src, dst_ref=dst, send_sem=ss, recv_sem=rs,
            device_id=(ds, dx), device_id_type=MESH,
        )

    def plane(d):
        q = (r + d) % R
        return q, z * R + q

    def across(e):
        q = (y + e) % Y * 2 + c
        return q, z * R + q

    def chunk(k, core):
        k = (k + core * ((z + 1) // 2)) % (z + 1)
        evens = (z + 2) // 2
        return jnp.where(k < evens, 2 * k, 2 * (k - evens) + 1)

    loads = [
        pltpu.make_async_copy(a, b, in_sem.at[i])
        for i, (a, b) in enumerate((
            (value_h, value), (go_h, go), (gate_h, gate), (w_h, w),
            (gain_h, gain), (shift_h, shift), (tbias_h, tbias),
        ))
    ]
    for load in loads:
        load.start()

    barrier = pltpu.get_barrier_semaphore()
    for d in range(1, R):
        q, dev = plane(d)
        pl.semaphore_signal(barrier, inc=1, device_id=(dev, x), device_id_type=MESH)
    for d in range(1, Z):
        pl.semaphore_signal(
            barrier, inc=1, device_id=((z + d) % Z * R + r, x), device_id_type=MESH
        )
    for d in range(1, X):
        pl.semaphore_signal(barrier, inc=1, device_id=(s, (x + d) % X), device_id_type=MESH)

    for load in loads[:3]:
        load.wait()
    v = value[...].astype(F32)
    gm = (go[...].astype(F32) * gate[...].astype(F32)).astype(BF16)
    g_all[r] = gm
    lane = lax.broadcasted_iota(jnp.int32, (T, T), 1)

    def as_rows(cols):
        m = jnp.zeros((T, T), F32)
        for i, col in enumerate(cols):
            m = jnp.where(lane == i, col, m)
        return m.T[:8]

    stat1[x] = as_rows((
        jnp.sum(v, axis=1, keepdims=True),
        jnp.sum(v * v, axis=1, keepdims=True),
        jnp.sum(gm.astype(F32), axis=1, keepdims=True),
    ))
    for load in loads[3:]:
        load.wait()
    with at("barrier"):
        pl.semaphore_wait(barrier, (R - 1) + (Z - 1) + (X - 1))

    def x_send(buf, ss, rs):
        for d in range(1, X):
            t = (x + d) % X
            rcopy(buf.at[x], buf.at[x], ss.at[d], rs.at[x], s, t).start()

    def x_wait(buf, ss, rs):
        for d in range(1, X):
            t = (x + d) % X
            cp = rcopy(buf.at[x], buf.at[t], ss.at[d], rs.at[t], s, t)
            cp.wait_recv()
            cp.wait_send()

    x_send(stat1, st_ss, st_rs)
    for e in (1, 3, 2):
        q, dev = across(e)
        rcopy(g_all.at[r], g_all.at[r], g_ss.at[e], g_rs.at[r], dev, x).start()
    rcopy(g_all.at[r], g_all.at[r], g_ss.at[4], g_rs.at[r], sib, x).start()

    def w_send(k, carry):
        for d in range(1, R):
            q, dev = plane(d)
            zz = chunk(k, q % 2)
            cols = pl.ds(pl.multiple_of((zz * R + q) * T, T), T)
            rcopy(w.at[:, cols], wt.at[zz, r], w_ss.at[zz, d], w_rs.at[zz, r], dev, x).start()
        return carry

    with at("w send"):
        lax.fori_loop(0, z + 1, w_send, 0)

    with at("stat wait"):
        x_wait(stat1, st_ss, st_rs)
    tot = stat1[0] + stat1[1] + stat1[2] + stat1[3]
    tb[...] = tot[2:3]
    colm = jnp.concatenate([tot[:3], tbias[...], jnp.zeros((T - 4, T), F32)], axis=0).T
    mean = colm[:, 0:1] / hidden
    var = colm[:, 1:2] / hidden - mean * mean
    inv = lax.rsqrt(var + 1e-05)
    centred = (v - mean) * inv
    cen[...] = centred
    rows[0] = jnp.broadcast_to(inv, (T, T))
    rows[1] = jnp.broadcast_to(colm[:, 3:4], (T, T))
    n_all[z] = (centred * gain[...] + shift[...]).astype(BF16)

    def n_send(k, carry):
        zz = Z - 1 - k
        rcopy(n_all.at[z], n_all.at[z], n_ss.at[zz], n_rs.at[z], zz * R + r, x).start()
        return carry

    with at("n send"):
        lax.fori_loop(0, Z - 1 - z, n_send, 0)

    with at("g wait"):
        for e in (1, 3, 2):
            q, dev = across(e)
            rcopy(g_all.at[q], g_all.at[q], g_ss.at[e], g_rs.at[q], dev, x).wait_recv()
            rcopy(g_all.at[q], g_all.at[q], g_ss.at[4 + e], g_rs.at[q], sib, x).start()
        for e in range(Y):
            q = (y + e) % Y * 2 + (1 - c)
            rcopy(g_all.at[q], g_all.at[q], g_ss.at[4], g_rs.at[q], sib, x).wait_recv()

    def grad_part(k):
        zz = chunk(k, c)
        with at("w wait"):
            for d in range(1, R):
                q, dev = plane(d)
                rcopy(wt.at[zz, q], wt.at[zz, q], w_ss.at[zz, d], w_rs.at[zz, q], dev, x).wait_recv()
        wt[zz, r] = w[:, pl.ds(pl.multiple_of((zz * R + r) * T, T), T)]

        @pl.when(zz == z)
        def _():
            row = lax.broadcasted_iota(jnp.int32, (T, T), 0)
            own = wt[zz, r].astype(F32)
            wt[zz, r] = jnp.where(row >= lane, own, 0.0).astype(BF16)

            def clear(q, carry):
                wt[zz, q] = jnp.zeros((T, T), BF16)
                return carry

            lax.fori_loop(0, r, clear, 0)

        gn = dot(wt[zz].reshape(R * T, T), g_all[...].reshape(R * T, -1), 0, 0)

        @pl.when(zz == z)
        def _():
            gn_own[...] = gn

        @pl.when(zz != z)
        def _():
            gn_send[zz] = gn.astype(BF16)
            rcopy(
                gn_send.at[zz], gn_recv.at[z], gn_ss.at[zz], gn_rs.at[z], zz * R + r, x
            ).start()

    def half(ref, h):
        return ref.at[pl.ds(pl.multiple_of(h * H, H), H), :]

    def norm_part(j):
        zz = chunk(j, c)

        @pl.when(zz != z)
        def _():
            with at("n wait"):
                rcopy(
                    n_all.at[zz], n_all.at[zz], n_ss.at[zz], n_rs.at[zz], zz * R + r, x
                ).wait_recv()

        nz = n_all[zz]
        gw_send[zz] = dot(g_all[...].reshape(R * T, -1), nz, 1, 1).astype(BF16)
        t = zz // 2
        role = (x - t + X) % X

        @pl.when(role == 2)
        def _():
            for h, e in ((0, 1), (1, 3)):
                rcopy(
                    half(gw_send.at[zz], h), gwo.at[zz], go_ss.at[zz, h], go_rs.at[zz],
                    s, (t + e) % X,
                ).start()

        @pl.when(role % 2 == 1)
        def _():
            side = role // 2
            h = 1 - side
            rcopy(
                half(gw_send.at[zz], h), half(gwx.at[zz % 2, side], h),
                gx_ss.at[zz, h], gx_rs.at[zz % 2, side, h], s, t,
            ).start()

        sp = dot(wt[zz].reshape(R * T, T), nz, 1, 0).reshape(R, T, -1)

        @pl.when(j == 0)
        def _():
            s_acc[...] = sp

        @pl.when(j > 0)
        def _():
            s_acc[...] += sp

    def pass_part(j):
        zz = chunk(j, c)
        t = zz // 2
        role = (x - t + X) % X

        @pl.when(role % 2 == 1)
        def _():
            side = role // 2
            with at("gwo wait"):
                rcopy(gwo.at[zz], gwo.at[zz], go_ss.at[zz, 0], go_rs.at[zz], s, t).wait_recv()
            mine = half(gw_send.at[zz], side)
            mine[...] = (mine[...].astype(F32) + gwo[zz].astype(F32)).astype(BF16)
            rcopy(
                mine, half(gwx.at[zz % 2, side], side),
                gx_ss.at[zz, side], gx_rs.at[zz % 2, side, side], s, t,
            ).start()

    lag = jnp.where(z >= 5, 1, z + 1)

    def step(k, carry):
        @pl.when(k <= z)
        def _():
            grad_part(k)

        @pl.when((k >= lag) & (k <= z + lag))
        def _():
            norm_part(k - lag)

        @pl.when(k >= lag + 1)
        def _():
            pass_part(k - lag - 1)

        return carry

    lax.fori_loop(0, z + lag + 2, step, 0)

    for e in range(Y):
        q = (y + e) % Y
        rcopy(s_acc.at[q * 2 + 1 - c], s_sib.at[q], sb_ss.at[q], sb_rs.at[q], sib, x).start()
    with at("sib wait"):
        for e in (1, 3, 2, 0):
            q, dev = across(e)
            p = (y + e) % Y
            rcopy(s_acc.at[q], s_sib.at[p], sb_ss.at[p], sb_rs.at[p], sib, x).wait_recv()
            if e:
                s_send[p] = (s_acc[q] + s_sib[p]).astype(BF16)
                rcopy(s_send.at[p], s_recv.at[y], s_ss.at[e], s_rs.at[y], dev, x).start()

    for b in range(2):
        zb = 2 * x + b

        @pl.when(zb <= z)
        def _():
            with at("gwx wait"):
                for side in range(2):
                    for h in range(2):
                        rcopy(
                            half(gw_send.at[zb], h), half(gwx.at[b, side], h),
                            gx_ss.at[zb, h], gx_rs.at[b, side, h], s, (x + 1 + 2 * side) % X,
                        ).wait_recv()
            gwr[b] = (
                gw_send[zb].astype(F32) + gwx[b, 0].astype(F32) + gwx[b, 1].astype(F32)
            ).astype(BF16).reshape(R, T, T)
            for d in range(1, R):
                q, dev = plane(d)
                rcopy(
                    gwr.at[b, q], gwf.at[b, r], gf_ss.at[b, d], gf_rs.at[b, r], dev, x
                ).start()
            gwf[b, r] = gwr[b, r]

        @pl.when(zb > z)
        def _():
            gwf[b] = jnp.zeros((R, T, T), BF16)

    acc = s_acc[r] + s_sib[y]
    with at("s wait"):
        for e in (1, 3, 2):
            p = (y + e) % Y
            q, dev = across(e)
            rcopy(s_send.at[p], s_recv.at[p], s_ss.at[e], s_rs.at[p], dev, x).wait_recv()
            acc = acc + s_recv[p].astype(F32)
    gg[...] = (go[...].astype(F32) * (acc + rows[1][:, 0:1])).astype(BF16)
    stores = [
        pltpu.make_async_copy(a, b, out_sem.at[i])
        for i, (a, b) in enumerate(
            ((gg, gg_out), (tb, tb_out), (gv, gv_out), (gw, gw_out), (gs, gs_out))
        )
    ]
    stores[0].start()
    stores[1].start()

    def gn_wait(k, carry):
        zz = z + 1 + k
        rcopy(
            gn_send.at[zz], gn_recv.at[zz], gn_ss.at[zz], gn_rs.at[zz], zz * R + r, x
        ).wait_recv()
        gn_own[...] += gn_recv[zz].astype(F32)
        return carry

    with at("gn wait"):
        lax.fori_loop(0, Z - 1 - z, gn_wait, 0)
    gn = gn_own[...]
    centred = cen[...]
    gc = gn * gain[...]
    stat2[x] = as_rows((
        jnp.sum(gc, axis=1, keepdims=True),
        jnp.sum(gc * centred, axis=1, keepdims=True),
    ))
    x_send(stat2, sp_ss, sp_rs)
    red1[r] = jnp.concatenate([
        jnp.sum(gn * centred, axis=0, keepdims=True),
        jnp.sum(gn, axis=0, keepdims=True),
        jnp.zeros((6, gn.shape[1]), F32),
    ], axis=0)
    for d in range(1, R):
        q, dev = plane(d)
        rcopy(red1.at[r], red1.at[r], ra_ss.at[d], ra_rs.at[r], dev, x).start()
    with at("red1 wait"):
        for d in range(1, R):
            q, dev = plane(d)
            cp = rcopy(red1.at[r], red1.at[q], ra_ss.at[d], ra_rs.at[q], dev, x)
            cp.wait_recv()
            cp.wait_send()
    tot = red1[0]
    for q in range(1, R):
        tot = tot + red1[q]
    red2[z] = tot
    for d in range(1, Z):
        zz = (z + d) % Z
        rcopy(red2.at[z], red2.at[z], rb_ss.at[d], rb_rs.at[z], zz * R + r, x).start()
    with at("stat2 wait"):
        x_wait(stat2, sp_ss, sp_rs)
    tot = stat2[0] + stat2[1] + stat2[2] + stat2[3]
    colm = jnp.concatenate([tot, jnp.zeros((T - 8, T), F32)], axis=0).T
    gv[...] = (
        rows[0][:, 0:1] * (gc - colm[:, 0:1] / hidden - centred * (colm[:, 1:2] / hidden))
    ).astype(BF16)
    stores[2].start()

    for b in range(2):
        zb = 2 * x + b

        @pl.when(zb <= z)
        def _():
            with at("gwf wait"):
                for d in range(1, R):
                    q, dev = plane(d)
                    cp = rcopy(gwr.at[b, q], gwf.at[b, q], gf_ss.at[b, d], gf_rs.at[b, q], dev, x)
                    cp.wait_recv()
                    cp.wait_send()

        for q in range(R):
            gw[:, (b * R + q) * T : (b * R + q + 1) * T] = gwf[b, q]
    stores[3].start()

    for e in range(1, Y):
        q, dev = across(e)
        rcopy(g_all.at[r], g_all.at[r], g_ss.at[e], g_rs.at[r], dev, x).wait_send()
        rcopy(g_all.at[r], g_all.at[r], g_ss.at[4 + e], g_rs.at[r], sib, x).wait_send()
        p = (y + e) % Y
        rcopy(s_send.at[p], s_recv.at[y], s_ss.at[e], s_rs.at[y], dev, x).wait_send()
    rcopy(g_all.at[r], g_all.at[r], g_ss.at[4], g_rs.at[r], sib, x).wait_send()
    for q in range(Y):
        rcopy(s_acc.at[q * 2 + 1 - c], s_sib.at[q], sb_ss.at[q], sb_rs.at[q], sib, x).wait_send()

    def drain_w(zz, carry):
        for d in range(1, R):
            q, dev = plane(d)
            rcopy(wt.at[zz, q], wt.at[zz, r], w_ss.at[zz, d], w_rs.at[zz, r], dev, x).wait_send()
        role = (x - zz // 2 + X) % X

        @pl.when(role == 2)
        def _():
            for h in range(2):
                rcopy(
                    half(gw_send.at[zz], h), gwo.at[zz], go_ss.at[zz, h], go_rs.at[zz], s,
                    (x + 1) % X,
                ).wait_send()

        @pl.when(role % 2 == 1)
        def _():
            for h in range(2):
                rcopy(
                    half(gw_send.at[zz], h), half(gwx.at[0, 0], h),
                    gx_ss.at[zz, h], gx_rs.at[0, 0, h], s, (x + 1) % X,
                ).wait_send()

        return carry

    lax.fori_loop(0, z + 1, drain_w, 0)

    def drain_gn(zz, carry):
        rcopy(
            gn_send.at[zz], gn_recv.at[z], gn_ss.at[zz], gn_rs.at[z], zz * R + r, x
        ).wait_send()
        return carry

    lax.fori_loop(0, z, drain_gn, 0)

    def drain_n(zz, carry):
        rcopy(n_all.at[z], n_all.at[z], n_ss.at[zz], n_rs.at[z], zz * R + r, x).wait_send()
        return carry

    lax.fori_loop(z + 1, Z, drain_n, 0)

    with at("red2 wait"):
        for d in range(1, Z):
            zz = (z + d) % Z
            cp = rcopy(red2.at[z], red2.at[zz], rb_ss.at[d], rb_rs.at[zz], zz * R + r, x)
            cp.wait_recv()
            cp.wait_send()
    tot = red2[0]
    for q in range(1, Z):
        tot = tot + red2[q]
    gs[...] = tot
    stores[4].start()
    for store in stores:
        store.wait()


def per_device(gate_half, value_half, norm_gain, norm_shift, token_weight, token_bias, grad_output):
    rows, chans = gate_half.shape
    cols = token_weight.shape[1]
    width = cols // X
    dma = pltpu.SemaphoreType.DMA
    gg, gv, gs, gw, tb = pl.pallas_call(
        functools.partial(kernel, chans * X),
        out_shape=(
            jax.ShapeDtypeStruct((rows, chans), BF16),
            jax.ShapeDtypeStruct((rows, chans), BF16),
            jax.ShapeDtypeStruct((8, chans), F32),
            jax.ShapeDtypeStruct((rows, width), BF16),
            jax.ShapeDtypeStruct((1, rows), F32),
        ),
        in_specs=[pl.BlockSpec(memory_space=pl.ANY)] * 7,
        out_specs=(pl.BlockSpec(memory_space=pl.ANY),) * 5,
        scratch_shapes=[
            pltpu.VMEM((R, T, chans), BF16),
            pltpu.VMEM((Z, T, chans), BF16),
            pltpu.VMEM((Z, R, T, T), BF16),
            pltpu.VMEM((R, T, chans), F32),
            pltpu.VMEM((Y, T, chans), F32),
            pltpu.VMEM((Y, T, chans), BF16),
            pltpu.VMEM((Y, T, chans), BF16),
            pltpu.VMEM((T, chans), F32),
            pltpu.VMEM((Z, T, chans), BF16),
            pltpu.VMEM((Z, T, chans), BF16),
            pltpu.VMEM((Z, R * T, T), BF16),
            pltpu.VMEM((Z, R * T // 2, T), BF16),
            pltpu.VMEM((2, 2, R * T, T), BF16),
            pltpu.VMEM((2, R, T, T), BF16),
            pltpu.VMEM((2, R, T, T), BF16),
            pltpu.VMEM((X, 8, T), F32),
            pltpu.VMEM((X, 8, T), F32),
            pltpu.VMEM((R, 8, chans), F32),
            pltpu.VMEM((Z, 8, chans), F32),
            pltpu.VMEM((T, chans), F32),
            pltpu.VMEM((2, T, T), F32),
            pltpu.VMEM((rows, chans), BF16),
            pltpu.VMEM((rows, chans), BF16),
            pltpu.VMEM((1, chans), F32),
            pltpu.VMEM((1, chans), F32),
            pltpu.VMEM((rows, cols), BF16),
            pltpu.VMEM((1, rows), F32),
            pltpu.VMEM((rows, chans), BF16),
            dma((7,)),
            pltpu.VMEM((rows, chans), BF16),
            pltpu.VMEM((rows, chans), BF16),
            pltpu.VMEM((8, chans), F32),
            pltpu.VMEM((rows, width), BF16),
            pltpu.VMEM((1, rows), F32),
            dma((5,)),
            dma((R,)), dma((R,)),
            dma((Z, R)), dma((Z, R)),
            dma((Z,)), dma((Z,)),
            dma((Y,)), dma((Y,)),
            dma((Y,)), dma((Y,)),
            dma((Z,)), dma((Z,)),
            dma((Z, 2)), dma((Z,)),
            dma((Z, 2)), dma((2, 2, 2)),
            dma((2, R)), dma((2, R)),
            dma((X,)), dma((X,)),
            dma((X,)), dma((X,)),
            dma((R,)), dma((R,)),
            dma((Z,)), dma((Z,)),
        ],
        compiler_params=pltpu.CompilerParams(
            collective_id=0, has_side_effects=True, vmem_limit_bytes=60 * 1024 * 1024
        ),
    )(
        gate_half, value_half, norm_gain[None], norm_shift[None], token_weight, token_bias[None],
        grad_output,
    )
    row = lax.axis_index("seq") * rows + lax.iota(jnp.int32, rows)[:, None]
    col = lax.axis_index("hid") * width + lax.iota(jnp.int32, width)[None, :]
    grad_weight = jnp.where(col <= row, gw.astype(F32), 0.0)
    return gg, gv, gs[0], gs[1], grad_weight, tb[0]


def solution(mesh):
    placed = (
        P("seq", "hid"),
        P("seq", "hid"),
        P("hid"),
        P("hid"),
        P("seq", None),
        P("seq"),
        P("seq", "hid"),
    )
    return jax.shard_map(
        per_device,
        mesh=mesh,
        in_specs=placed,
        out_specs=(P("seq", "hid"), P("seq", "hid"), P("hid"), P("hid"), P("seq", "hid"), P("seq")),
        check_vma=False,
    )
```

```python
import contextlib
import functools

import jax
import jax.numpy as jnp
from jax import lax
from jax.experimental import pallas as pl
from jax.experimental.pallas import tpu as pltpu
from jax.sharding import PartitionSpec as P

MESH = pl.DeviceIdType.MESH
F32 = jnp.float32
BF16 = jnp.bfloat16
T = 128
R = 8
Z = 8
X = 4
Y = 4


def at(name):
    return contextlib.nullcontext()


def dot(a, b, ca, cb):
    return lax.dot_general(a, b, (((ca,), (cb,)), ((), ())), preferred_element_type=F32)


def kernel(
    hidden,
    gate_h, value_h, gain_h, shift_h, w_h, tbias_h, go_h,
    gg_out, gv_out, gs_out, gw_out, tb_out,
    g_all, n_all, wt, s_acc, s_sib, s_send, s_recv, gn_own, gn_send, gn_recv,
    gw_send, gwo, gwx, gwr, gwf,
    stat1, stat2, red1, red2, cen, rows,
    gate, value, gain, shift, w, tbias, go, in_sem,
    gg, gv, gs, tb, out_sem, gw_sem,
    g_ss, g_rs, gb_rs, w_ss, w_rs, f_ss, f_rs, n_ss, n_rs, sb_ss, sb_rs, s_ss, s_rs, gn_ss, gn_rs,
    go_ss, go_rs, gx_ss, gx_rs, gf_ss, gf_rs,
    st_ss, st_rs, sp_ss, sp_rs, ra_ss, ra_rs, rb_ss, rb_rs,
):
    s = lax.axis_index("seq")
    x = lax.axis_index("hid")
    z = s // R
    r = s % R
    y = r // 2
    c = r % 2
    sib = z * R + y * 2 + (1 - c)
    H = R * T // 2

    def rcopy(src, dst, ss, rs, ds, dx):
        return pltpu.make_async_remote_copy(
            src_ref=src, dst_ref=dst, send_sem=ss, recv_sem=rs,
            device_id=(ds, dx), device_id_type=MESH,
        )

    def plane(d):
        q = (r + d) % R
        return q, z * R + q

    def across(e):
        q = (y + e) % Y * 2 + c
        return q, z * R + q

    def chunk(k, core):
        p = (k + core * ((z + 1) // 2)) % (z + 1)
        evens = (z + 2) // 2
        p = z - jnp.where(p < evens, 2 * p, 2 * (p - evens) + 1)
        return jnp.where(k > z, z + 1, p)

    n_shared = jnp.maximum(z - (Z // 2 - 1), 0)
    quarter = pl.ds(pl.multiple_of(x * (T // X), T // X), T // X)

    def shared(k):
        return (k % 2 == 0) & (k < 2 * n_shared)

    def columns(zz, q):
        return pl.ds(pl.multiple_of((zz * R + q) * T, T), T)

    def share_send(m, carry):
        for d in range(1, R):
            q, dev = plane(d)
            zz = chunk(2 * m, q % 2)
            rcopy(
                w.at[quarter, columns(zz, q)], wt.at[zz, r, quarter],
                w_ss.at[2 * m], w_rs.at[zz], dev, x,
            ).start()
        zz = chunk(2 * m, c)
        wt[zz, r, quarter] = w[quarter, columns(zz, r)]
        return carry

    def share_pass(m, carry):
        zz = chunk(2 * m, c)
        got = wt.at[zz, 1:, quarter]
        rcopy(got, got, w_ss.at[zz], w_rs.at[zz], sib, x).wait_recv()
        for d in range(1, X):
            t = (x + d) % X
            part = wt.at[zz, :, quarter]
            rcopy(part, part, f_ss.at[zz], f_rs.at[zz], s, t).start()
        return carry

    loads = [
        pltpu.make_async_copy(a, b, in_sem.at[i])
        for i, (a, b) in enumerate((
            (value_h, value), (go_h, go), (gate_h, gate), (w_h, w),
            (gain_h, gain), (shift_h, shift), (tbias_h, tbias),
        ))
    ]
    for load in loads:
        load.start()

    barrier = pltpu.get_barrier_semaphore()
    for d in range(1, R):
        q, dev = plane(d)
        pl.semaphore_signal(barrier, inc=1, device_id=(dev, x), device_id_type=MESH)
    for d in range(1, Z):
        pl.semaphore_signal(
            barrier, inc=1, device_id=((z + d) % Z * R + r, x), device_id_type=MESH
        )
    for d in range(1, X):
        pl.semaphore_signal(barrier, inc=1, device_id=(s, (x + d) % X), device_id_type=MESH)

    for load in loads[:3]:
        load.wait()
    v = value[...].astype(F32)
    gm = (go[...].astype(F32) * gate[...].astype(F32)).astype(BF16)
    g_all[r] = gm
    lane = lax.broadcasted_iota(jnp.int32, (T, T), 1)

    def as_rows(cols):
        m = jnp.zeros((T, T), F32)
        for i, col in enumerate(cols):
            m = jnp.where(lane == i, col, m)
        return m.T[:8]

    stat1[x] = as_rows((
        jnp.sum(v, axis=1, keepdims=True),
        jnp.sum(v * v, axis=1, keepdims=True),
        jnp.sum(gm.astype(F32), axis=1, keepdims=True),
    ))
    for load in loads[3:]:
        load.wait()
    with at("barrier"):
        pl.semaphore_wait(barrier, (R - 1) + (Z - 1) + (X - 1))

    def x_send(buf, ss, rs):
        for d in range(1, X):
            t = (x + d) % X
            rcopy(buf.at[x], buf.at[x], ss, rs, s, t).start()

    def x_wait(buf, ss, rs):
        cp = rcopy(buf.at[1:], buf.at[1:], ss, rs, sib, x)
        cp.wait_recv()
        cp.wait_send()

    x_send(stat1, st_ss, st_rs)
    lax.fori_loop(0, n_shared, share_send, 0)
    for e in (1, 3, 2):
        q, dev = across(e)
        rcopy(g_all.at[r], g_all.at[r], g_ss, g_rs.at[r], dev, x).start()
    rcopy(g_all.at[r], g_all.at[r], g_ss, gb_rs, sib, x).start()

    def w_send(k, carry):
        @pl.when(jnp.logical_not(shared(k)))
        def _():
            for d in range(1, R):
                q, dev = plane(d)
                zz = chunk(k, q % 2)
                rcopy(
                    w.at[:, columns(zz, q)], wt.at[zz, r], w_ss.at[k], w_rs.at[zz], dev, x
                ).start()

        return carry

    with at("w send"):
        lax.fori_loop(0, z + 1, w_send, 0)

    with at("stat wait"):
        x_wait(stat1, st_ss, st_rs)
    tot = stat1[0] + stat1[1] + stat1[2] + stat1[3]
    tb[...] = tot[2:3]
    colm = jnp.concatenate([tot[:3], tbias[...], jnp.zeros((T - 4, T), F32)], axis=0).T
    mean = colm[:, 0:1] / hidden
    var = colm[:, 1:2] / hidden - mean * mean
    inv = lax.rsqrt(var + 1e-05)
    centred = (v - mean) * inv
    cen[...] = centred
    rows[0] = jnp.broadcast_to(inv, (T, T))
    rows[1] = jnp.broadcast_to(colm[:, 3:4], (T, T))
    n_all[z] = (centred * gain[...] + shift[...]).astype(BF16)

    with at("n send"):
        for d in (1, 7, 2, 6, 3, 5, 4):
            zz = z + d

            @pl.when(zz < Z)
            def _():
                rcopy(n_all.at[z], n_all.at[z], n_ss.at[zz], n_rs.at[z], zz * R + r, x).start()

    with at("share pass"):
        lax.fori_loop(0, n_shared, share_pass, 0)

    with at("g wait"):
        for e in (1, 3, 2):
            q, dev = across(e)
            rcopy(g_all.at[q], g_all.at[q], g_ss, g_rs.at[q], dev, x).wait_recv()
            rcopy(g_all.at[q], g_all.at[q], g_ss, gb_rs, sib, x).start()
        rcopy(g_all.at[Y:], g_all.at[Y:], g_ss, gb_rs, sib, x).wait_recv()

    def arrive(k):
        zz = chunk(k, c)

        @pl.when(shared(k))
        def _():
            with at("share wait"):
                got = wt.at[zz, :, : T - T // X]
                cp = rcopy(got, got, f_ss.at[zz], f_rs.at[zz], sib, x)
                cp.wait_recv()
                cp.wait_send()

        @pl.when(jnp.logical_not(shared(k)) & (k <= z))
        def _():
            with at("w wait"):
                got = wt.at[zz, 1:]
                rcopy(got, got, w_ss.at[zz], w_rs.at[zz], sib, x).wait_recv()
            wt[zz, r] = w[:, columns(zz, r)]

        @pl.when(zz == z)
        def _():
            row = lax.broadcasted_iota(jnp.int32, (T, T), 0)
            own = wt[zz, r].astype(F32)
            wt[zz, r] = jnp.where(row >= lane, own, 0.0).astype(BF16)

            def clear(q, carry):
                wt[zz, q] = jnp.zeros((T, T), BF16)
                return carry

            lax.fori_loop(0, r, clear, 0)

        return zz

    def both(a, b):
        return jnp.concatenate([wt[a].reshape(R * T, T), wt[b].reshape(R * T, T)], axis=1)

    def grad_part(p):
        pair = arrive(2 * p), arrive(2 * p + 1)
        gn = dot(both(*pair), g_all[...].reshape(R * T, -1), 0, 0)
        for i, zz in enumerate(pair):
            part = gn[i * T : (i + 1) * T]

            @pl.when(zz == z)
            def _():
                gn_own[...] = part

            @pl.when(zz < z)
            def _():
                gn_send[zz] = part.astype(BF16)
                rcopy(
                    gn_send.at[zz], gn_recv.at[z], gn_ss.at[zz], gn_rs.at[z], zz * R + r, x
                ).start()

    def half(ref, h):
        return ref.at[pl.ds(pl.multiple_of(h * H, H), H), :]

    def norm_part(p):
        pair = chunk(2 * p, c), chunk(2 * p + 1, c)
        for zz in pair:

            @pl.when(zz < z)
            def _():
                with at("n wait"):
                    rcopy(
                        n_all.at[zz], n_all.at[zz], n_ss.at[zz], n_rs.at[zz], zz * R + r, x
                    ).wait_recv()

        nz = jnp.concatenate([n_all[pair[0]], n_all[pair[1]]], axis=0)
        prod = dot(g_all[...].reshape(R * T, -1), nz, 1, 1).astype(BF16)
        for i, zz in enumerate(pair):
            gw_send[zz] = prod[:, i * T : (i + 1) * T]
            t = zz // 2
            role = (x - t + X) % X

            @pl.when((role == 2) & (zz <= z))
            def _():
                for h, e in ((0, 1), (1, 3)):
                    rcopy(
                        half(gw_send.at[zz], h), gwo.at[zz], go_ss.at[zz, h], go_rs.at[zz],
                        s, (t + e) % X,
                    ).start()

            @pl.when((role % 2 == 1) & (zz <= z))
            def _():
                side = role // 2
                h = 1 - side
                rcopy(
                    half(gw_send.at[zz], h), half(gwx.at[zz % 2, side], h),
                    gx_ss.at[zz, h], gx_rs.at[zz % 2, side, h], s, t,
                ).start()

        sp = dot(both(*pair), nz, 1, 0).reshape(R, T, -1)

        @pl.when(p == 0)
        def _():
            s_acc[...] = sp

        @pl.when(p > 0)
        def _():
            s_acc[...] += sp

    def pass_part(j):
        zz = chunk(j, c)
        t = zz // 2
        role = (x - t + X) % X

        @pl.when((role % 2 == 1) & (zz <= z))
        def _():
            side = role // 2
            with at("gwo wait"):
                rcopy(gwo.at[zz], gwo.at[zz], go_ss.at[zz, 0], go_rs.at[zz], s, t).wait_recv()
            mine = half(gw_send.at[zz], side)
            mine[...] = (mine[...].astype(F32) + gwo[zz].astype(F32)).astype(BF16)
            rcopy(
                mine, half(gwx.at[zz % 2, side], side),
                gx_ss.at[zz, side], gx_rs.at[zz % 2, side, side], s, t,
            ).start()

    @pl.when(z % 2 == 0)
    def _():
        wt[z + 1] = jnp.zeros((R, T, T), BF16)
        n_all[z + 1] = jnp.zeros((T, n_all.shape[2]), BF16)

    pairs = (z + 2) // 2

    def step(k, carry):
        @pl.when(k < pairs)
        def _():
            grad_part(k)

        @pl.when((k >= 1) & (k <= pairs))
        def _():
            norm_part(k - 1)

        @pl.when(k >= 2)
        def _():
            pass_part(2 * (k - 2))
            pass_part(2 * (k - 2) + 1)

        return carry

    lax.fori_loop(0, pairs + 2, step, 0)

    stores = [
        pltpu.make_async_copy(a, b, out_sem.at[i])
        for i, (a, b) in enumerate(((gg, gg_out), (tb, tb_out), (gv, gv_out), (gs, gs_out)))
    ]
    stores[1].start()

    for e in range(Y):
        q = (y + e) % Y
        rcopy(s_acc.at[q * 2 + 1 - c], s_sib.at[q], sb_ss, sb_rs.at[q], sib, x).start()
    def grad_normed():
        def gn_wait(k, carry):
            zz = z + 1 + k
            rcopy(
                gn_send.at[zz], gn_recv.at[zz], gn_ss.at[zz], gn_rs.at[zz], zz * R + r, x
            ).wait_recv()
            gn_own[...] += gn_recv[zz].astype(F32)
            return carry

        with at("gn wait"):
            lax.fori_loop(0, Z - 1 - z, gn_wait, 0)
        gn = gn_own[...]
        centred = cen[...]
        gc = gn * gain[...]
        stat2[x] = as_rows((
            jnp.sum(gc, axis=1, keepdims=True),
            jnp.sum(gc * centred, axis=1, keepdims=True),
        ))
        x_send(stat2, sp_ss, sp_rs)
        red1[r] = jnp.concatenate([
            jnp.sum(gn * centred, axis=0, keepdims=True),
            jnp.sum(gn, axis=0, keepdims=True),
            jnp.zeros((6, gn.shape[1]), F32),
        ], axis=0)
        for d in range(1, R):
            q, dev = plane(d)
            rcopy(red1.at[r], red1.at[r], ra_ss, ra_rs, dev, x).start()
    @pl.when(z >= 6)
    def _():
        grad_normed()

    with at("sib wait"):
        for e in (1, 3, 2, 0):
            q, dev = across(e)
            p = (y + e) % Y
            rcopy(s_acc.at[q], s_sib.at[p], sb_ss, sb_rs.at[p], sib, x).wait_recv()
            if e:
                s_send[p] = (s_acc[q] + s_sib[p]).astype(BF16)
                rcopy(s_send.at[p], s_recv.at[y], s_ss, s_rs.at[y], dev, x).start()

    @pl.when(z < 6)
    def _():
        grad_normed()

    for b in range(2):
        zb = 2 * x + b

        @pl.when(zb <= z)
        def _():
            with at("gwx wait"):
                for side in range(2):
                    for h in range(2):
                        rcopy(
                            half(gw_send.at[zb], h), half(gwx.at[b, side], h),
                            gx_ss.at[zb, h], gx_rs.at[b, side, h], s, (x + 1 + 2 * side) % X,
                        ).wait_recv()
            gwr[b] = (
                gw_send[zb].astype(F32) + gwx[b, 0].astype(F32) + gwx[b, 1].astype(F32)
            ).astype(BF16).reshape(R, T, T)
            for d in range(1, R):
                q, dev = plane(d)
                rcopy(
                    gwr.at[b, q], gwf.at[b, r], gf_ss.at[b], gf_rs.at[b], dev, x
                ).start()
            gwf[b, r] = gwr[b, r]

        @pl.when(zb > z)
        def _():
            gwf[b] = jnp.zeros((R, T, T), BF16)

    with at("red1 wait"):
        cp = rcopy(red1.at[1:], red1.at[1:], ra_ss, ra_rs, sib, x)
        cp.wait_recv()
        cp.wait_send()
    tot = red1[0]
    for q in range(1, R):
        tot = tot + red1[q]
    red2[z] = tot
    for d in range(1, Z):
        zz = (z + d) % Z
        rcopy(red2.at[z], red2.at[z], rb_ss, rb_rs, zz * R + r, x).start()
    acc = s_acc[r] + s_sib[y]
    with at("s wait"):
        for e in (1, 3, 2):
            p = (y + e) % Y
            q, dev = across(e)
            rcopy(s_send.at[p], s_recv.at[p], s_ss, s_rs.at[p], dev, x).wait_recv()
            acc = acc + s_recv[p].astype(F32)
    gg[...] = (go[...].astype(F32) * (acc + rows[1][:, 0:1])).astype(BF16)
    stores[0].start()

    with at("stat2 wait"):
        x_wait(stat2, sp_ss, sp_rs)
    tot = stat2[0] + stat2[1] + stat2[2] + stat2[3]
    colm = jnp.concatenate([tot, jnp.zeros((T - 8, T), F32)], axis=0).T
    centred = cen[...]
    gc = gn_own[...] * gain[...]
    gv[...] = (
        rows[0][:, 0:1] * (gc - colm[:, 0:1] / hidden - centred * (colm[:, 1:2] / hidden))
    ).astype(BF16)
    stores[2].start()


    for b in range(2):
        zb = 2 * x + b

        @pl.when(zb <= z)
        def _():
            with at("gwf wait"):
                cp = rcopy(gwr.at[b, 1:], gwf.at[b, 1:], gf_ss.at[b], gf_rs.at[b], sib, x)
                cp.wait_recv()
                cp.wait_send()

        for q in range(R):
            some = pl.ds((b * R + q) * T, T)
            pltpu.make_async_copy(gwf.at[b, q], gw_out.at[:, some], gw_sem).start()

    rcopy(s_send.at[1:], s_recv.at[1:], s_ss, s_rs.at[0], sib, x).wait_send()
    rcopy(g_all.at[1:], g_all.at[1:], g_ss, gb_rs, sib, x).wait_send()
    rcopy(s_sib, s_sib, sb_ss, sb_rs.at[0], sib, x).wait_send()

    def drain_w(k, carry):
        @pl.when(shared(k))
        def _():
            sent = wt.at[0, 1:, quarter]
            rcopy(sent, sent, w_ss.at[k], w_rs.at[0], sib, x).wait_send()

        @pl.when(jnp.logical_not(shared(k)))
        def _():
            sent = wt.at[0, 1:]
            rcopy(sent, sent, w_ss.at[k], w_rs.at[0], sib, x).wait_send()

        zz = k
        role = (x - zz // 2 + X) % X

        @pl.when(role == 2)
        def _():
            for h in range(2):
                rcopy(
                    half(gw_send.at[zz], h), gwo.at[zz], go_ss.at[zz, h], go_rs.at[zz], s,
                    (x + 1) % X,
                ).wait_send()

        @pl.when(role % 2 == 1)
        def _():
            for h in range(2):
                rcopy(
                    half(gw_send.at[zz], h), half(gwx.at[0, 0], h),
                    gx_ss.at[zz, h], gx_rs.at[0, 0, h], s, (x + 1) % X,
                ).wait_send()

        return carry

    with at("drain"):
        lax.fori_loop(0, z + 1, drain_w, 0)

    def drain_gn(zz, carry):
        rcopy(
            gn_send.at[zz], gn_recv.at[z], gn_ss.at[zz], gn_rs.at[z], zz * R + r, x
        ).wait_send()
        return carry

    lax.fori_loop(0, z, drain_gn, 0)

    def drain_n(zz, carry):
        rcopy(n_all.at[z], n_all.at[z], n_ss.at[zz], n_rs.at[z], zz * R + r, x).wait_send()
        return carry

    lax.fori_loop(z + 1, Z, drain_n, 0)

    with at("red2 wait"):
        cp = rcopy(red2.at[1:], red2.at[1:], rb_ss, rb_rs, sib, x)
        cp.wait_recv()
        cp.wait_send()
    tot = red2[0]
    for q in range(1, Z):
        tot = tot + red2[q]
    gs[...] = tot
    stores[3].start()
    with at("store wait"):
        for store in stores:
            store.wait()
        pltpu.make_async_copy(gwf, gwf, gw_sem).wait()


def finish(
    gg_in, gv_in, gs_in, gw_in, tb_in, gg_out, gv_out, gain_out, shift_out, gw_out, tb_out,
    gg, gv, gs, gw, tb, gw_f, in_sem, sem,
):
    rows, width = gw_f.shape
    loads = [
        pltpu.make_async_copy(a, b, in_sem.at[i])
        for i, (a, b) in enumerate(
            ((gw_in, gw), (gg_in, gg), (gv_in, gv), (gs_in, gs), (tb_in, tb))
        )
    ]
    for load in loads:
        load.start()
    row = lax.axis_index("seq") * rows + lax.broadcasted_iota(jnp.int32, (rows, T), 0)
    lane = lax.axis_index("hid") * width + lax.broadcasted_iota(jnp.int32, (rows, T), 1)
    loads[0].wait()
    copies = []
    for q in range(width // T):
        cols = slice(q * T, (q + 1) * T)
        gw_f[:, cols] = jnp.where(lane + q * T <= row, gw[:, cols].astype(F32), 0.0)
        if q % 4 == 3:
            some = pl.ds((q - 3) * T, 4 * T)
            copies.append(
                pltpu.make_async_copy(gw_f.at[:, some], gw_out.at[:, some], sem.at[5 + q // 4])
            )
            copies[-1].start()
        if q == 3:
            for load in loads[1:]:
                load.wait()
            for i, (a, b) in enumerate((
                (gg, gg_out), (gv, gv_out), (tb, tb_out),
                (gs.at[0:1], gain_out), (gs.at[1:2], shift_out),
            )):
                copies.append(pltpu.make_async_copy(a, b, sem.at[i]))
                copies[-1].start()
    for copy in copies:
        copy.wait()


def per_device(gate_half, value_half, norm_gain, norm_shift, token_weight, token_bias, grad_output):
    rows, chans = gate_half.shape
    cols = token_weight.shape[1]
    width = cols // X
    dma = pltpu.SemaphoreType.DMA
    anywhere = pl.BlockSpec(memory_space=pl.ANY)
    gg, gv, gs, gw, tb = pl.pallas_call(
        functools.partial(kernel, chans * X),
        out_shape=(
            jax.ShapeDtypeStruct((rows, chans), BF16),
            jax.ShapeDtypeStruct((rows, chans), BF16),
            jax.ShapeDtypeStruct((8, chans), F32),
            jax.ShapeDtypeStruct((rows, width), BF16),
            jax.ShapeDtypeStruct((1, rows), F32),
        ),
        in_specs=[anywhere] * 7,
        out_specs=(anywhere,) * 5,
        scratch_shapes=[
            pltpu.VMEM((R, T, chans), BF16),
            pltpu.VMEM((Z, T, chans), BF16),
            pltpu.VMEM((Z, R, T, T), BF16),
            pltpu.VMEM((R, T, chans), F32),
            pltpu.VMEM((Y, T, chans), F32),
            pltpu.VMEM((Y, T, chans), BF16),
            pltpu.VMEM((Y, T, chans), BF16),
            pltpu.VMEM((T, chans), F32),
            pltpu.VMEM((Z, T, chans), BF16),
            pltpu.VMEM((Z, T, chans), BF16),
            pltpu.VMEM((Z, R * T, T), BF16),
            pltpu.VMEM((Z, R * T // 2, T), BF16),
            pltpu.VMEM((2, 2, R * T, T), BF16),
            pltpu.VMEM((2, R, T, T), BF16),
            pltpu.VMEM((2, R, T, T), BF16),
            pltpu.VMEM((X, 8, T), F32),
            pltpu.VMEM((X, 8, T), F32),
            pltpu.VMEM((R, 8, chans), F32),
            pltpu.VMEM((Z, 8, chans), F32),
            pltpu.VMEM((T, chans), F32),
            pltpu.VMEM((2, T, T), F32),
            pltpu.VMEM((rows, chans), BF16),
            pltpu.VMEM((rows, chans), BF16),
            pltpu.VMEM((1, chans), F32),
            pltpu.VMEM((1, chans), F32),
            pltpu.VMEM((rows, cols), BF16),
            pltpu.VMEM((1, rows), F32),
            pltpu.VMEM((rows, chans), BF16),
            dma((7,)),
            pltpu.VMEM((rows, chans), BF16),
            pltpu.VMEM((rows, chans), BF16),
            pltpu.VMEM((8, chans), F32),
            pltpu.VMEM((1, rows), F32),
            dma((4,)), dma(()),
            dma(()), dma((R,)), dma(()),
            dma((Z,)), dma((Z,)),
            dma((Z,)), dma((Z,)),
            dma((Z,)), dma((Z,)),
            dma(()), dma((Y,)),
            dma(()), dma((Y,)),
            dma((Z,)), dma((Z,)),
            dma((Z, 2)), dma((Z,)),
            dma((Z, 2)), dma((2, 2, 2)),
            dma((2,)), dma((2,)),
            *([dma(())] * 8),
        ],
        compiler_params=pltpu.CompilerParams(
            collective_id=0, has_side_effects=True, vmem_limit_bytes=60 * 1024 * 1024
        ),
    )(
        gate_half, value_half, norm_gain[None], norm_shift[None], token_weight, token_bias[None],
        grad_output,
    )
    gg, gv, gain, shift, gw, tb = pl.pallas_call(
        finish,
        out_shape=(
            jax.ShapeDtypeStruct((rows, chans), BF16),
            jax.ShapeDtypeStruct((rows, chans), BF16),
            jax.ShapeDtypeStruct((1, chans), F32),
            jax.ShapeDtypeStruct((1, chans), F32),
            jax.ShapeDtypeStruct((rows, width), F32),
            jax.ShapeDtypeStruct((1, rows), F32),
        ),
        in_specs=[anywhere] * 5,
        out_specs=(anywhere,) * 6,
        scratch_shapes=[
            pltpu.VMEM((rows, chans), BF16),
            pltpu.VMEM((rows, chans), BF16),
            pltpu.VMEM((8, chans), F32),
            pltpu.VMEM((rows, width), BF16),
            pltpu.VMEM((1, rows), F32),
            pltpu.VMEM((rows, width), F32),
            dma((5,)),
            dma((5 + width // T // 4,)),
        ],
        compiler_params=pltpu.CompilerParams(vmem_limit_bytes=60 * 1024 * 1024),
    )(gg, gv, gs, gw, tb)
    return gg, gv, gain[0], shift[0], gw, tb[0]


def solution(mesh):
    placed = (
        P("seq", "hid"),
        P("seq", "hid"),
        P("hid"),
        P("hid"),
        P("seq", None),
        P("seq"),
        P("seq", "hid"),
    )
    return jax.shard_map(
        per_device,
        mesh=mesh,
        in_specs=placed,
        out_specs=(P("seq", "hid"), P("seq", "hid"), P("hid"), P("hid"), P("seq", "hid"), P("seq")),
        check_vma=False,
    )
```

```python
import contextlib
import functools

import jax
import jax.numpy as jnp
from jax import lax
from jax.experimental import pallas as pl
from jax.experimental.pallas import tpu as pltpu
from jax.sharding import PartitionSpec as P

MESH = pl.DeviceIdType.MESH
F32 = jnp.float32
BF16 = jnp.bfloat16
T = 128
R = 8
Z = 8
X = 4
Y = 4


def at(name):
    return contextlib.nullcontext()


def dot(a, b, ca, cb):
    return lax.dot_general(a, b, (((ca,), (cb,)), ((), ())), preferred_element_type=F32)


def kernel(
    hidden,
    gate_h, value_h, gain_h, shift_h, w_h, tbias_h, go_h,
    gg_out, gv_out, gs_out, gw_out, tb_out,
    g_all, n_all, wt, s_acc, s_sib, s_send, s_recv, gn_own, gn_send, gn_recv,
    gw_send, gwo, gwx, gwr, gwf,
    stat1, stat2, red1, red2, cen, rows,
    gate, value, gain, shift, w, tbias, go, in_sem,
    gg, gv, gs, tb, out_sem, gw_sem,
    g_ss, g_rs, gb_rs, w_ss, w_rs, f_ss, f_rs, n_ss, n_rs, sb_ss, sb_rs, s_ss, s_rs, gn_ss, gn_rs,
    go_ss, go_rs, gx_ss, gx_rs, gf_ss, gf_rs,
    st_ss, st_rs, sp_ss, sp_rs, ra_ss, ra_rs, rb_ss, rb_rs,
):
    s = lax.axis_index("seq")
    x = lax.axis_index("hid")
    z = s // R
    r = s % R
    y = r // 2
    c = r % 2
    sib = z * R + y * 2 + (1 - c)
    H = R * T // 2

    def rcopy(src, dst, ss, rs, ds, dx):
        return pltpu.make_async_remote_copy(
            src_ref=src, dst_ref=dst, send_sem=ss, recv_sem=rs,
            device_id=(ds, dx), device_id_type=MESH,
        )

    def plane(d):
        q = (r + d) % R
        return q, z * R + q

    def across(e):
        q = (y + e) % Y * 2 + c
        return q, z * R + q

    def chunk(k, core):
        p = (k + core * ((z + 1) // 2)) % (z + 1)
        evens = (z + 2) // 2
        p = z - jnp.where(p < evens, 2 * p, 2 * (p - evens) + 1)
        return jnp.where(k > z, z + 1, p)

    n_shared = jnp.maximum(z - Z // 2, 0)
    quarter = pl.ds(pl.multiple_of(x * (T // X), T // X), T // X)

    def shared(k):
        return (k % 2 == 0) & (k < 2 * n_shared)

    def columns(zz, q):
        return pl.ds(pl.multiple_of((zz * R + q) * T, T), T)

    def share_send(m, carry):
        for d in range(1, R):
            q, dev = plane(d)
            zz = chunk(2 * m, q % 2)
            rcopy(
                w.at[quarter, columns(zz, q)], wt.at[zz, r, quarter],
                w_ss.at[2 * m], w_rs.at[zz], dev, x,
            ).start()
        zz = chunk(2 * m, c)
        wt[zz, r, quarter] = w[quarter, columns(zz, r)]
        return carry

    def share_pass(m, carry):
        zz = chunk(2 * m, c)
        got = wt.at[zz, 1:, quarter]
        rcopy(got, got, w_ss.at[zz], w_rs.at[zz], sib, x).wait_recv()
        for d in range(1, X):
            t = (x + d) % X
            part = wt.at[zz, :, quarter]
            rcopy(part, part, f_ss.at[zz], f_rs.at[zz], s, t).start()
        return carry

    loads = [
        pltpu.make_async_copy(a, b, in_sem.at[i])
        for i, (a, b) in enumerate((
            (value_h, value), (go_h, go), (gate_h, gate), (w_h, w),
            (gain_h, gain), (shift_h, shift), (tbias_h, tbias),
        ))
    ]
    for load in loads:
        load.start()

    barrier = pltpu.get_barrier_semaphore()
    for d in range(1, R):
        q, dev = plane(d)
        pl.semaphore_signal(barrier, inc=1, device_id=(dev, x), device_id_type=MESH)
    for d in range(1, Z):
        pl.semaphore_signal(
            barrier, inc=1, device_id=((z + d) % Z * R + r, x), device_id_type=MESH
        )
    for d in range(1, X):
        pl.semaphore_signal(barrier, inc=1, device_id=(s, (x + d) % X), device_id_type=MESH)

    for load in loads[:3]:
        load.wait()
    v = value[...].astype(F32)
    gm = (go[...].astype(F32) * gate[...].astype(F32)).astype(BF16)
    g_all[r] = gm
    lane = lax.broadcasted_iota(jnp.int32, (T, T), 1)

    def as_rows(cols):
        m = jnp.zeros((T, T), F32)
        for i, col in enumerate(cols):
            m = jnp.where(lane == i, col, m)
        return m.T[:8]

    stat1[x] = as_rows((
        jnp.sum(v, axis=1, keepdims=True),
        jnp.sum(v * v, axis=1, keepdims=True),
        jnp.sum(gm.astype(F32), axis=1, keepdims=True),
    ))
    for load in loads[3:]:
        load.wait()
    with at("barrier"):
        pl.semaphore_wait(barrier, (R - 1) + (Z - 1) + (X - 1))

    def x_send(buf, ss, rs):
        for d in range(1, X):
            t = (x + d) % X
            rcopy(buf.at[x], buf.at[x], ss, rs, s, t).start()

    def x_wait(buf, ss, rs):
        cp = rcopy(buf.at[1:], buf.at[1:], ss, rs, sib, x)
        cp.wait_recv()
        cp.wait_send()

    x_send(stat1, st_ss, st_rs)
    lax.fori_loop(0, n_shared, share_send, 0)
    for e in (1, 3, 2):
        q, dev = across(e)
        rcopy(g_all.at[r], g_all.at[r], g_ss, g_rs.at[r], dev, x).start()
    rcopy(g_all.at[r], g_all.at[r], g_ss, gb_rs, sib, x).start()

    def w_send(k, carry):
        @pl.when(jnp.logical_not(shared(k)))
        def _():
            for d in range(1, R):
                q, dev = plane(d)
                zz = chunk(k, q % 2)
                rcopy(
                    w.at[:, columns(zz, q)], wt.at[zz, r], w_ss.at[k], w_rs.at[zz], dev, x
                ).start()

        return carry

    with at("w send"):
        lax.fori_loop(0, z + 1, w_send, 0)

    with at("stat wait"):
        x_wait(stat1, st_ss, st_rs)
    tot = stat1[0] + stat1[1] + stat1[2] + stat1[3]
    tb[...] = tot[2:3]
    colm = jnp.concatenate([tot[:3], tbias[...], jnp.zeros((T - 4, T), F32)], axis=0).T
    mean = colm[:, 0:1] / hidden
    var = colm[:, 1:2] / hidden - mean * mean
    inv = lax.rsqrt(var + 1e-05)
    centred = (v - mean) * inv
    cen[...] = centred
    rows[0] = jnp.broadcast_to(inv, (T, T))
    rows[1] = jnp.broadcast_to(colm[:, 3:4], (T, T))
    n_all[z] = (centred * gain[...] + shift[...]).astype(BF16)

    with at("n send"):
        for d in (1, 7, 2, 6, 3, 5, 4):
            zz = z + d

            @pl.when(zz < Z)
            def _():
                rcopy(n_all.at[z], n_all.at[z], n_ss.at[zz], n_rs.at[z], zz * R + r, x).start()

    with at("share pass"):
        lax.fori_loop(0, n_shared, share_pass, 0)

    with at("g wait"):
        for e in (1, 3, 2):
            q, dev = across(e)
            rcopy(g_all.at[q], g_all.at[q], g_ss, g_rs.at[q], dev, x).wait_recv()
            rcopy(g_all.at[q], g_all.at[q], g_ss, gb_rs, sib, x).start()
        rcopy(g_all.at[Y:], g_all.at[Y:], g_ss, gb_rs, sib, x).wait_recv()

    def arrive(k):
        zz = chunk(k, c)

        @pl.when(shared(k))
        def _():
            with at("share wait"):
                got = wt.at[zz, :, : T - T // X]
                cp = rcopy(got, got, f_ss.at[zz], f_rs.at[zz], sib, x)
                cp.wait_recv()
                cp.wait_send()

        @pl.when(jnp.logical_not(shared(k)) & (k <= z))
        def _():
            with at("w wait"):
                got = wt.at[zz, 1:]
                rcopy(got, got, w_ss.at[zz], w_rs.at[zz], sib, x).wait_recv()
            wt[zz, r] = w[:, columns(zz, r)]

        @pl.when(zz == z)
        def _():
            row = lax.broadcasted_iota(jnp.int32, (T, T), 0)
            own = wt[zz, r].astype(F32)
            wt[zz, r] = jnp.where(row >= lane, own, 0.0).astype(BF16)

            def clear(q, carry):
                wt[zz, q] = jnp.zeros((T, T), BF16)
                return carry

            lax.fori_loop(0, r, clear, 0)

        return zz

    def both(a, b):
        return jnp.concatenate([wt[a].reshape(R * T, T), wt[b].reshape(R * T, T)], axis=1)

    def grad_part(p):
        pair = arrive(2 * p), arrive(2 * p + 1)
        gn = dot(both(*pair), g_all[...].reshape(R * T, -1), 0, 0)
        for i, zz in enumerate(pair):
            part = gn[i * T : (i + 1) * T]

            @pl.when(zz == z)
            def _():
                gn_own[...] = part

            far = z - zz

            @pl.when(far > 0)
            def _():
                gn_send[zz] = part.astype(BF16)

            @pl.when(far >= 1)
            def _():
                rcopy(
                    gn_send.at[zz], gn_recv.at[z], gn_ss.at[zz], gn_rs.at[z], zz * R + r, x
                ).start()

    def half(ref, h):
        return ref.at[pl.ds(pl.multiple_of(h * H, H), H), :]

    def norm_part(p):
        pair = chunk(2 * p, c), chunk(2 * p + 1, c)

        for zz in pair:

            @pl.when(zz < z)
            def _():
                with at("n wait"):
                    rcopy(
                        n_all.at[zz], n_all.at[zz], n_ss.at[zz], n_rs.at[zz], zz * R + r, x
                    ).wait_recv()

        nz = jnp.concatenate([n_all[pair[0]], n_all[pair[1]]], axis=0)
        prod = dot(g_all[...].reshape(R * T, -1), nz, 1, 1).astype(BF16)
        for i, zz in enumerate(pair):
            gw_send[zz] = prod[:, i * T : (i + 1) * T]
            t = zz // 2
            role = (x - t + X) % X

            @pl.when((role == 2) & (zz <= z))
            def _():
                for h, e in ((0, 1), (1, 3)):
                    rcopy(
                        half(gw_send.at[zz], h), gwo.at[zz], go_ss.at[zz, h], go_rs.at[zz],
                        s, (t + e) % X,
                    ).start()

            @pl.when((role % 2 == 1) & (zz <= z))
            def _():
                side = role // 2
                h = 1 - side
                rcopy(
                    half(gw_send.at[zz], h), half(gwx.at[zz % 2, side], h),
                    gx_ss.at[zz, h], gx_rs.at[zz % 2, side, h], s, t,
                ).start()

        sp = dot(both(*pair), nz, 1, 0).reshape(R, T, -1)

        @pl.when(p == 0)
        def _():
            s_acc[...] = sp

        @pl.when(p > 0)
        def _():
            s_acc[...] += sp

    def pass_part(j):
        zz = chunk(j, c)
        t = zz // 2
        role = (x - t + X) % X

        @pl.when((role % 2 == 1) & (zz <= z))
        def _():
            side = role // 2
            with at("gwo wait"):
                rcopy(gwo.at[zz], gwo.at[zz], go_ss.at[zz, 0], go_rs.at[zz], s, t).wait_recv()
            mine = half(gw_send.at[zz], side)
            mine[...] = (mine[...].astype(F32) + gwo[zz].astype(F32)).astype(BF16)
            rcopy(
                mine, half(gwx.at[zz % 2, side], side),
                gx_ss.at[zz, side], gx_rs.at[zz % 2, side, side], s, t,
            ).start()

    @pl.when(z % 2 == 0)
    def _():
        wt[z + 1] = jnp.zeros((R, T, T), BF16)
        n_all[z + 1] = jnp.zeros((T, n_all.shape[2]), BF16)

    pairs = (z + 2) // 2
    lag = jnp.where(z == Z - 1, 1, 2)

    def step(k, carry):
        @pl.when(k < pairs)
        def _():
            grad_part(k)

        @pl.when((k >= lag) & (k < pairs + lag))
        def _():
            norm_part(k - lag)

        @pl.when(k >= lag + 2)
        def _():
            pass_pair(k - lag - 2, 0)

        return carry

    def pass_pair(p, carry):
        pass_part(2 * p)
        pass_part(2 * p + 1)
        return carry

    lax.fori_loop(0, pairs + lag, step, 0)

    stores = [
        pltpu.make_async_copy(a, b, out_sem.at[i])
        for i, (a, b) in enumerate(((gg, gg_out), (tb, tb_out), (gv, gv_out), (gs, gs_out)))
    ]
    stores[1].start()

    for e in range(Y):
        q = (y + e) % Y
        rcopy(s_acc.at[q * 2 + 1 - c], s_sib.at[q], sb_ss, sb_rs.at[q], sib, x).start()
    def grad_normed():
        with at("gn wait"):
            for d in range(1, Z):
                zz = z + d

                @pl.when(zz < Z)
                def _():
                    rcopy(
                        gn_send.at[0], gn_recv.at[zz], gn_ss.at[0], gn_rs.at[zz], sib, x
                    ).wait_recv()
                    gn_own[...] += gn_recv[zz].astype(F32)

        gn = gn_own[...]
        centred = cen[...]
        gc = gn * gain[...]
        stat2[x] = as_rows((
            jnp.sum(gc, axis=1, keepdims=True),
            jnp.sum(gc * centred, axis=1, keepdims=True),
        ))
        x_send(stat2, sp_ss, sp_rs)
        red1[r] = jnp.concatenate([
            jnp.sum(gn * centred, axis=0, keepdims=True),
            jnp.sum(gn, axis=0, keepdims=True),
            jnp.zeros((6, gn.shape[1]), F32),
        ], axis=0)
        for d in range(1, R):
            q, dev = plane(d)
            rcopy(red1.at[r], red1.at[r], ra_ss, ra_rs, dev, x).start()
    @pl.when(z >= 6)
    def _():
        grad_normed()

    with at("sib wait"):
        for e in (1, 3, 2, 0):
            q, dev = across(e)
            p = (y + e) % Y
            rcopy(s_acc.at[q], s_sib.at[p], sb_ss, sb_rs.at[p], sib, x).wait_recv()
            if e:
                s_send[p] = (s_acc[q] + s_sib[p]).astype(BF16)
                rcopy(s_send.at[p], s_recv.at[y], s_ss, s_rs.at[y], dev, x).start()

    def collect():
        for b in range(2):
            zb = 2 * x + b

            @pl.when(zb <= z)
            def _():
                with at("gwx wait"):
                    for side in range(2):
                        for h in range(2):
                            rcopy(
                                half(gw_send.at[zb], h), half(gwx.at[b, side], h),
                                gx_ss.at[zb, h], gx_rs.at[b, side, h], s, (x + 1 + 2 * side) % X,
                            ).wait_recv()
                gwr[b] = (
                    gw_send[zb].astype(F32) + gwx[b, 0].astype(F32) + gwx[b, 1].astype(F32)
                ).astype(BF16).reshape(R, T, T)
                for d in range(1, R):
                    q, dev = plane(d)
                    rcopy(
                        gwr.at[b, q], gwf.at[b, r], gf_ss.at[b], gf_rs.at[b], dev, x
                    ).start()
                gwf[b, r] = gwr[b, r]

            @pl.when(zb > z)
            def _():
                gwf[b] = jnp.zeros((R, T, T), BF16)

    lax.fori_loop(jnp.maximum(pairs - 2, 0), pairs, pass_pair, 0)

    @pl.when(z < Z // 2)
    def _():
        collect()

    @pl.when(z < 6)
    def _():
        grad_normed()

    @pl.when(z >= Z // 2)
    def _():
        collect()

    with at("red1 wait"):
        cp = rcopy(red1.at[1:], red1.at[1:], ra_ss, ra_rs, sib, x)
        cp.wait_recv()
        cp.wait_send()
    tot = red1[0]
    for q in range(1, R):
        tot = tot + red1[q]
    red2[z] = tot
    for d in range(1, Z):
        zz = (z + d) % Z
        rcopy(red2.at[z], red2.at[z], rb_ss, rb_rs, zz * R + r, x).start()
    acc = s_acc[r] + s_sib[y]
    with at("s wait"):
        for e in (1, 3, 2):
            p = (y + e) % Y
            q, dev = across(e)
            rcopy(s_send.at[p], s_recv.at[p], s_ss, s_rs.at[p], dev, x).wait_recv()
            acc = acc + s_recv[p].astype(F32)
    gg[...] = (go[...].astype(F32) * (acc + rows[1][:, 0:1])).astype(BF16)
    stores[0].start()

    with at("stat2 wait"):
        x_wait(stat2, sp_ss, sp_rs)
    tot = stat2[0] + stat2[1] + stat2[2] + stat2[3]
    colm = jnp.concatenate([tot, jnp.zeros((T - 8, T), F32)], axis=0).T
    centred = cen[...]
    gc = gn_own[...] * gain[...]
    gv[...] = (
        rows[0][:, 0:1] * (gc - colm[:, 0:1] / hidden - centred * (colm[:, 1:2] / hidden))
    ).astype(BF16)
    stores[2].start()


    for b in range(2):
        zb = 2 * x + b

        @pl.when(zb <= z)
        def _():
            with at("gwf wait"):
                cp = rcopy(gwr.at[b, 1:], gwf.at[b, 1:], gf_ss.at[b], gf_rs.at[b], sib, x)
                cp.wait_recv()
                cp.wait_send()

        for q in range(R):
            some = pl.ds((b * R + q) * T, T)
            pltpu.make_async_copy(gwf.at[b, q], gw_out.at[:, some], gw_sem).start()

    rcopy(s_send.at[1:], s_recv.at[1:], s_ss, s_rs.at[0], sib, x).wait_send()
    rcopy(g_all.at[1:], g_all.at[1:], g_ss, gb_rs, sib, x).wait_send()
    rcopy(s_sib, s_sib, sb_ss, sb_rs.at[0], sib, x).wait_send()

    def drain_w(k, carry):
        @pl.when(shared(k))
        def _():
            sent = wt.at[0, 1:, quarter]
            rcopy(sent, sent, w_ss.at[k], w_rs.at[0], sib, x).wait_send()

        @pl.when(jnp.logical_not(shared(k)))
        def _():
            sent = wt.at[0, 1:]
            rcopy(sent, sent, w_ss.at[k], w_rs.at[0], sib, x).wait_send()

        zz = k
        role = (x - zz // 2 + X) % X

        @pl.when(role == 2)
        def _():
            for h in range(2):
                rcopy(
                    half(gw_send.at[zz], h), gwo.at[zz], go_ss.at[zz, h], go_rs.at[zz], s,
                    (x + 1) % X,
                ).wait_send()

        @pl.when(role % 2 == 1)
        def _():
            for h in range(2):
                rcopy(
                    half(gw_send.at[zz], h), half(gwx.at[0, 0], h),
                    gx_ss.at[zz, h], gx_rs.at[0, 0, h], s, (x + 1) % X,
                ).wait_send()

        return carry

    with at("drain"):
        lax.fori_loop(0, z + 1, drain_w, 0)

    def drain_gn(zz, carry):
        rcopy(
            gn_send.at[zz], gn_recv.at[z], gn_ss.at[zz], gn_rs.at[z], zz * R + r, x
        ).wait_send()
        return carry

    lax.fori_loop(0, z, drain_gn, 0)

    for d in range(1, Z):

        @pl.when(z + d < Z)
        def _():
            rcopy(n_all.at[z], n_all.at[z], n_ss.at[z + d], n_rs.at[z], sib, x).wait_send()

    with at("red2 wait"):
        cp = rcopy(red2.at[1:], red2.at[1:], rb_ss, rb_rs, sib, x)
        cp.wait_recv()
        cp.wait_send()
    tot = red2[0]
    for q in range(1, Z):
        tot = tot + red2[q]
    gs[...] = tot
    stores[3].start()
    with at("store wait"):
        for store in stores:
            store.wait()
        pltpu.make_async_copy(gwf, gwf, gw_sem).wait()


def finish(
    gg_in, gv_in, gs_in, gw_in, tb_in, gg_out, gv_out, gain_out, shift_out, gw_out, tb_out,
    gg, gv, gs, gw, tb, gw_f, in_sem, sem,
):
    rows, width = gw_f.shape
    loads = [
        pltpu.make_async_copy(a, b, in_sem.at[i])
        for i, (a, b) in enumerate(
            ((gw_in, gw), (gg_in, gg), (gv_in, gv), (gs_in, gs), (tb_in, tb))
        )
    ]
    for load in loads:
        load.start()
    row = lax.axis_index("seq") * rows + lax.broadcasted_iota(jnp.int32, (rows, T), 0)
    lane = lax.axis_index("hid") * width + lax.broadcasted_iota(jnp.int32, (rows, T), 1)
    loads[0].wait()
    copies = []
    for q in range(width // T):
        cols = slice(q * T, (q + 1) * T)
        gw_f[:, cols] = jnp.where(lane + q * T <= row, gw[:, cols].astype(F32), 0.0)
        if q % 4 == 3:
            some = pl.ds((q - 3) * T, 4 * T)
            copies.append(
                pltpu.make_async_copy(gw_f.at[:, some], gw_out.at[:, some], sem.at[5 + q // 4])
            )
            copies[-1].start()
        if q == 3:
            for load in loads[1:]:
                load.wait()
            for i, (a, b) in enumerate((
                (gg, gg_out), (gv, gv_out), (tb, tb_out),
                (gs.at[0:1], gain_out), (gs.at[1:2], shift_out),
            )):
                copies.append(pltpu.make_async_copy(a, b, sem.at[i]))
                copies[-1].start()
    for copy in copies:
        copy.wait()


def per_device(gate_half, value_half, norm_gain, norm_shift, token_weight, token_bias, grad_output):
    rows, chans = gate_half.shape
    cols = token_weight.shape[1]
    width = cols // X
    dma = pltpu.SemaphoreType.DMA
    anywhere = pl.BlockSpec(memory_space=pl.ANY)
    gg, gv, gs, gw, tb = pl.pallas_call(
        functools.partial(kernel, chans * X),
        out_shape=(
            jax.ShapeDtypeStruct((rows, chans), BF16),
            jax.ShapeDtypeStruct((rows, chans), BF16),
            jax.ShapeDtypeStruct((8, chans), F32),
            jax.ShapeDtypeStruct((rows, width), BF16),
            jax.ShapeDtypeStruct((1, rows), F32),
        ),
        in_specs=[anywhere] * 7,
        out_specs=(anywhere,) * 5,
        scratch_shapes=[
            pltpu.VMEM((R, T, chans), BF16),
            pltpu.VMEM((Z, T, chans), BF16),
            pltpu.VMEM((Z, R, T, T), BF16),
            pltpu.VMEM((R, T, chans), F32),
            pltpu.VMEM((Y, T, chans), F32),
            pltpu.VMEM((Y, T, chans), BF16),
            pltpu.VMEM((Y, T, chans), BF16),
            pltpu.VMEM((T, chans), F32),
            pltpu.VMEM((Z, T, chans), BF16),
            pltpu.VMEM((Z, T, chans), BF16),
            pltpu.VMEM((Z, R * T, T), BF16),
            pltpu.VMEM((Z, R * T // 2, T), BF16),
            pltpu.VMEM((2, 2, R * T, T), BF16),
            pltpu.VMEM((2, R, T, T), BF16),
            pltpu.VMEM((2, R, T, T), BF16),
            pltpu.VMEM((X, 8, T), F32),
            pltpu.VMEM((X, 8, T), F32),
            pltpu.VMEM((R, 8, chans), F32),
            pltpu.VMEM((Z, 8, chans), F32),
            pltpu.VMEM((T, chans), F32),
            pltpu.VMEM((2, T, T), F32),
            pltpu.VMEM((rows, chans), BF16),
            pltpu.VMEM((rows, chans), BF16),
            pltpu.VMEM((1, chans), F32),
            pltpu.VMEM((1, chans), F32),
            pltpu.VMEM((rows, cols), BF16),
            pltpu.VMEM((1, rows), F32),
            pltpu.VMEM((rows, chans), BF16),
            dma((7,)),
            pltpu.VMEM((rows, chans), BF16),
            pltpu.VMEM((rows, chans), BF16),
            pltpu.VMEM((8, chans), F32),
            pltpu.VMEM((1, rows), F32),
            dma((4,)), dma(()),
            dma(()), dma((R,)), dma(()),
            dma((Z,)), dma((Z,)),
            dma((Z,)), dma((Z,)),
            dma((Z,)), dma((Z,)),
            dma(()), dma((Y,)),
            dma(()), dma((Y,)),
            dma((Z,)), dma((Z,)),
            dma((Z, 2)), dma((Z,)),
            dma((Z, 2)), dma((2, 2, 2)),
            dma((2,)), dma((2,)),
            *([dma(())] * 8),
        ],
        compiler_params=pltpu.CompilerParams(
            collective_id=0, has_side_effects=True, vmem_limit_bytes=60 * 1024 * 1024
        ),
    )(
        gate_half, value_half, norm_gain[None], norm_shift[None], token_weight, token_bias[None],
        grad_output,
    )
    gg, gv, gain, shift, gw, tb = pl.pallas_call(
        finish,
        out_shape=(
            jax.ShapeDtypeStruct((rows, chans), BF16),
            jax.ShapeDtypeStruct((rows, chans), BF16),
            jax.ShapeDtypeStruct((1, chans), F32),
            jax.ShapeDtypeStruct((1, chans), F32),
            jax.ShapeDtypeStruct((rows, width), F32),
            jax.ShapeDtypeStruct((1, rows), F32),
        ),
        in_specs=[anywhere] * 5,
        out_specs=(anywhere,) * 6,
        scratch_shapes=[
            pltpu.VMEM((rows, chans), BF16),
            pltpu.VMEM((rows, chans), BF16),
            pltpu.VMEM((8, chans), F32),
            pltpu.VMEM((rows, width), BF16),
            pltpu.VMEM((1, rows), F32),
            pltpu.VMEM((rows, width), F32),
            dma((5,)),
            dma((5 + width // T // 4,)),
        ],
        compiler_params=pltpu.CompilerParams(vmem_limit_bytes=60 * 1024 * 1024),
    )(gg, gv, gs, gw, tb)
    return gg, gv, gain[0], shift[0], gw, tb[0]


def solution(mesh):
    placed = (
        P("seq", "hid"),
        P("seq", "hid"),
        P("hid"),
        P("hid"),
        P("seq", None),
        P("seq"),
        P("seq", "hid"),
    )
    return jax.shard_map(
        per_device,
        mesh=mesh,
        in_specs=placed,
        out_specs=(P("seq", "hid"), P("seq", "hid"), P("hid"), P("hid"), P("seq", "hid"), P("seq")),
        check_vma=False,
    )
```

```python
import contextlib
import functools

import jax
import jax.numpy as jnp
from jax import lax
from jax.experimental import pallas as pl
from jax.experimental.pallas import tpu as pltpu
from jax.sharding import PartitionSpec as P

MESH = pl.DeviceIdType.MESH
F32 = jnp.float32
BF16 = jnp.bfloat16
T = 128
R = 8
Z = 8
X = 4
Y = 4


def at(name):
    return contextlib.nullcontext()


def dot(a, b, ca, cb):
    return lax.dot_general(a, b, (((ca,), (cb,)), ((), ())), preferred_element_type=F32)


def kernel(
    hidden,
    gate_h, value_h, gain_h, shift_h, w_h, tbias_h, go_h,
    gg_out, gv_out, gs_out, gw_out, tb_out,
    g_all, n_all, wt, s_acc, s_sib, s_send, s_recv, gn_own, gn_send, gn_recv,
    gw_send, gwo, gwx, gwr, gwf,
    stat1, stat2, red1, red2, cen, rows,
    gate, value, gain, shift, w, tbias, go, in_sem,
    gg, gv, gs, tb, out_sem, gw_sem,
    g_ss, g_rs, gb_rs, w_ss, w_rs, f_ss, f_rs, n_ss, n_rs, sb_ss, sb_rs, s_ss, s_rs, gn_ss, gn_rs,
    go_ss, go_rs, gx_ss, gx_rs, gf_ss, gf_rs,
    st_ss, st_rs, sp_ss, sp_rs, ra_ss, ra_rs, rb_ss, rb_rs,
):
    s = lax.axis_index("seq")
    x = lax.axis_index("hid")
    z = s // R
    r = s % R
    y = r // 2
    c = r % 2
    sib = z * R + y * 2 + (1 - c)
    H = R * T // 2

    def rcopy(src, dst, ss, rs, ds, dx):
        return pltpu.make_async_remote_copy(
            src_ref=src, dst_ref=dst, send_sem=ss, recv_sem=rs,
            device_id=(ds, dx), device_id_type=MESH,
        )

    def plane(d):
        q = (r + d) % R
        return q, z * R + q

    def across(e):
        q = (y + e) % Y * 2 + c
        return q, z * R + q

    def chunk(k, core):
        p = (k + core * ((z + 1) // 2)) % (z + 1)
        evens = (z + 2) // 2
        p = z - jnp.where(p < evens, 2 * p, 2 * (p - evens) + 1)
        return jnp.where(k > z, z + 1, p)

    n_shared = jnp.maximum(z - Z // 2, 0)
    quarter = pl.ds(pl.multiple_of(x * (T // X), T // X), T // X)

    def shared(k):
        return (k % 2 == 0) & (k < 2 * n_shared)

    def columns(zz, q):
        return pl.ds(pl.multiple_of((zz * R + q) * T, T), T)

    def share_send(m, carry):
        for d in range(1, R):
            q, dev = plane(d)
            zz = chunk(2 * m, q % 2)
            rcopy(
                w.at[quarter, columns(zz, q)], wt.at[zz, r, quarter],
                w_ss.at[2 * m], w_rs.at[zz], dev, x,
            ).start()
        zz = chunk(2 * m, c)
        wt[zz, r, quarter] = w[quarter, columns(zz, r)]
        return carry

    def share_pass(m, carry):
        zz = chunk(2 * m, c)
        got = wt.at[zz, 1:, quarter]
        rcopy(got, got, w_ss.at[zz], w_rs.at[zz], sib, x).wait_recv()
        for d in range(1, X):
            t = (x + d) % X
            part = wt.at[zz, :, quarter]
            rcopy(part, part, f_ss.at[zz], f_rs.at[zz], s, t).start()
        return carry

    loads = [
        pltpu.make_async_copy(a, b, in_sem.at[i])
        for i, (a, b) in enumerate((
            (value_h, value), (go_h, go), (gate_h, gate), (w_h, w),
            (gain_h, gain), (shift_h, shift), (tbias_h, tbias),
        ))
    ]
    for load in loads:
        load.start()

    barrier = pltpu.get_barrier_semaphore()
    for d in range(1, R):
        q, dev = plane(d)
        pl.semaphore_signal(barrier, inc=1, device_id=(dev, x), device_id_type=MESH)
    for d in range(1, Z):
        pl.semaphore_signal(
            barrier, inc=1, device_id=((z + d) % Z * R + r, x), device_id_type=MESH
        )
    for d in range(1, X):
        pl.semaphore_signal(barrier, inc=1, device_id=(s, (x + d) % X), device_id_type=MESH)

    for load in loads[:3]:
        load.wait()
    v = value[...].astype(F32)
    gm = (go[...].astype(F32) * gate[...].astype(F32)).astype(BF16)
    g_all[r] = gm
    lane = lax.broadcasted_iota(jnp.int32, (T, T), 1)

    def as_rows(cols):
        m = jnp.zeros((T, T), F32)
        for i, col in enumerate(cols):
            m = jnp.where(lane == i, col, m)
        return m.T[:8]

    stat1[x] = as_rows((
        jnp.sum(v, axis=1, keepdims=True),
        jnp.sum(v * v, axis=1, keepdims=True),
        jnp.sum(gm.astype(F32), axis=1, keepdims=True),
    ))
    for load in loads[3:]:
        load.wait()
    with at("barrier"):
        pl.semaphore_wait(barrier, (R - 1) + (Z - 1) + (X - 1))

    def x_send(buf, ss, rs):
        for d in range(1, X):
            t = (x + d) % X
            rcopy(buf.at[x], buf.at[x], ss, rs, s, t).start()

    def x_wait(buf, ss, rs):
        cp = rcopy(buf.at[1:], buf.at[1:], ss, rs, sib, x)
        cp.wait_recv()
        cp.wait_send()

    x_send(stat1, st_ss, st_rs)
    lax.fori_loop(0, n_shared, share_send, 0)
    for e in (1, 3, 2):
        q, dev = across(e)
        rcopy(g_all.at[r], g_all.at[r], g_ss, g_rs.at[r], dev, x).start()
    rcopy(g_all.at[r], g_all.at[r], g_ss, gb_rs, sib, x).start()

    def w_send(k, carry):
        @pl.when(jnp.logical_not(shared(k)))
        def _():
            for d in range(1, R):
                q, dev = plane(d)
                zz = chunk(k, q % 2)
                rcopy(
                    w.at[:, columns(zz, q)], wt.at[zz, r], w_ss.at[k], w_rs.at[zz], dev, x
                ).start()

        return carry

    with at("w send"):
        lax.fori_loop(0, z + 1, w_send, 0)

    with at("stat wait"):
        x_wait(stat1, st_ss, st_rs)
    tot = stat1[0] + stat1[1] + stat1[2] + stat1[3]
    tb[...] = tot[2:3]
    colm = jnp.concatenate([tot[:3], tbias[...], jnp.zeros((T - 4, T), F32)], axis=0).T
    mean = colm[:, 0:1] / hidden
    var = colm[:, 1:2] / hidden - mean * mean
    inv = lax.rsqrt(var + 1e-05)
    centred = (v - mean) * inv
    cen[...] = centred
    rows[0] = jnp.broadcast_to(inv, (T, T))
    rows[1] = jnp.broadcast_to(colm[:, 3:4], (T, T))
    n_all[z] = (centred * gain[...] + shift[...]).astype(BF16)

    with at("n send"):
        for d in (1, 7, 2, 6, 3, 5, 4):
            zz = z + d

            @pl.when(zz < Z)
            def _():
                rcopy(n_all.at[z], n_all.at[z], n_ss.at[zz], n_rs.at[z], zz * R + r, x).start()

    with at("share pass"):
        lax.fori_loop(0, n_shared, share_pass, 0)

    with at("g wait"):
        for e in (1, 3, 2):
            q, dev = across(e)
            rcopy(g_all.at[q], g_all.at[q], g_ss, g_rs.at[q], dev, x).wait_recv()
            rcopy(g_all.at[q], g_all.at[q], g_ss, gb_rs, sib, x).start()
        rcopy(g_all.at[Y:], g_all.at[Y:], g_ss, gb_rs, sib, x).wait_recv()

    def arrive(k):
        zz = chunk(k, c)

        @pl.when(shared(k))
        def _():
            with at("share wait"):
                got = wt.at[zz, :, : T - T // X]
                cp = rcopy(got, got, f_ss.at[zz], f_rs.at[zz], sib, x)
                cp.wait_recv()
                cp.wait_send()

        @pl.when(jnp.logical_not(shared(k)) & (k <= z))
        def _():
            with at("w wait"):
                got = wt.at[zz, 1:]
                rcopy(got, got, w_ss.at[zz], w_rs.at[zz], sib, x).wait_recv()
            wt[zz, r] = w[:, columns(zz, r)]

        @pl.when(zz == z)
        def _():
            row = lax.broadcasted_iota(jnp.int32, (T, T), 0)
            own = wt[zz, r].astype(F32)
            wt[zz, r] = jnp.where(row >= lane, own, 0.0).astype(BF16)

            def clear(q, carry):
                wt[zz, q] = jnp.zeros((T, T), BF16)
                return carry

            lax.fori_loop(0, r, clear, 0)

        return zz

    def both(a, b):
        return jnp.concatenate([wt[a].reshape(R * T, T), wt[b].reshape(R * T, T)], axis=1)

    def grad_part(p):
        pair = arrive(2 * p), arrive(2 * p + 1)
        gn = dot(both(*pair), g_all[...].reshape(R * T, -1), 0, 0)
        for i, zz in enumerate(pair):
            part = gn[i * T : (i + 1) * T]

            @pl.when(zz == z)
            def _():
                gn_own[...] = part

            far = z - zz

            @pl.when(far > 0)
            def _():
                gn_send[zz] = part.astype(BF16)

            @pl.when(far >= 1)
            def _():
                rcopy(
                    gn_send.at[zz], gn_recv.at[z], gn_ss.at[zz], gn_rs.at[z], zz * R + r, x
                ).start()

    def half(ref, h):
        return ref.at[pl.ds(pl.multiple_of(h * H, H), H), :]

    def norm_part(p):
        pair = chunk(2 * p, c), chunk(2 * p + 1, c)

        for zz in pair:

            @pl.when(zz < z)
            def _():
                with at("n wait"):
                    rcopy(
                        n_all.at[zz], n_all.at[zz], n_ss.at[zz], n_rs.at[zz], zz * R + r, x
                    ).wait_recv()

        nz = jnp.concatenate([n_all[pair[0]], n_all[pair[1]]], axis=0)
        prod = dot(g_all[...].reshape(R * T, -1), nz, 1, 1).astype(BF16)
        for i, zz in enumerate(pair):
            gw_send[zz] = prod[:, i * T : (i + 1) * T]
            t = zz // 2
            role = (x - t + X) % X

            @pl.when((role == 2) & (zz <= z))
            def _():
                for h, e in ((0, 1), (1, 3)):
                    rcopy(
                        half(gw_send.at[zz], h), gwo.at[zz], go_ss.at[zz], go_rs.at[zz],
                        s, (t + e) % X,
                    ).start()

            @pl.when((role % 2 == 1) & (zz <= z))
            def _():
                side = role // 2
                h = 1 - side
                rcopy(
                    half(gw_send.at[zz], h), half(gwx.at[zz % 2, side], h),
                    gx_ss.at[zz], gx_rs.at[zz % 2, side, h], s, t,
                ).start()

        sp = dot(both(*pair), nz, 1, 0).reshape(R, T, -1)

        @pl.when(p == 0)
        def _():
            s_acc[...] = sp

        @pl.when(p > 0)
        def _():
            s_acc[...] += sp

    def pass_part(j):
        zz = chunk(j, c)
        t = zz // 2
        role = (x - t + X) % X

        @pl.when((role % 2 == 1) & (zz <= z))
        def _():
            side = role // 2
            with at("gwo wait"):
                rcopy(gwo.at[zz], gwo.at[zz], go_ss.at[zz], go_rs.at[zz], s, t).wait_recv()
            mine = half(gw_send.at[zz], side)
            mine[...] = (mine[...].astype(F32) + gwo[zz].astype(F32)).astype(BF16)
            rcopy(
                mine, half(gwx.at[zz % 2, side], side),
                gx_ss.at[zz], gx_rs.at[zz % 2, side, side], s, t,
            ).start()

    @pl.when(z % 2 == 0)
    def _():
        wt[z + 1] = jnp.zeros((R, T, T), BF16)
        n_all[z + 1] = jnp.zeros((T, n_all.shape[2]), BF16)

    pairs = (z + 2) // 2
    lag = jnp.where(z == Z - 1, 1, 2)

    def step(k, carry):
        @pl.when(k < pairs)
        def _():
            grad_part(k)

        @pl.when((k >= lag) & (k < pairs + lag))
        def _():
            norm_part(k - lag)

        @pl.when(k >= lag + 2)
        def _():
            pass_pair(k - lag - 2, 0)

        return carry

    def pass_pair(p, carry):
        pass_part(2 * p)
        pass_part(2 * p + 1)
        return carry

    lax.fori_loop(0, pairs + lag, step, 0)

    stores = [
        pltpu.make_async_copy(a, b, out_sem.at[i])
        for i, (a, b) in enumerate(((gg, gg_out), (tb, tb_out), (gv, gv_out), (gs, gs_out)))
    ]
    stores[1].start()

    for e in range(Y):
        q = (y + e) % Y
        rcopy(s_acc.at[q * 2 + 1 - c], s_sib.at[q], sb_ss, sb_rs.at[q], sib, x).start()
    def grad_normed():
        with at("gn wait"):
            for d in range(1, Z):
                zz = z + d

                @pl.when(zz < Z)
                def _():
                    rcopy(
                        gn_send.at[0], gn_recv.at[zz], gn_ss.at[0], gn_rs.at[zz], sib, x
                    ).wait_recv()
                    gn_own[...] += gn_recv[zz].astype(F32)

        gn = gn_own[...]
        centred = cen[...]
        gc = gn * gain[...]
        stat2[x] = as_rows((
            jnp.sum(gc, axis=1, keepdims=True),
            jnp.sum(gc * centred, axis=1, keepdims=True),
        ))
        x_send(stat2, sp_ss, sp_rs)
        red1[r] = jnp.concatenate([
            jnp.sum(gn * centred, axis=0, keepdims=True),
            jnp.sum(gn, axis=0, keepdims=True),
        ], axis=0)
        for d in range(1, R):
            q, dev = plane(d)
            rcopy(red1.at[r], red1.at[r], ra_ss, ra_rs, dev, x).start()
    @pl.when(z >= 6)
    def _():
        grad_normed()

    with at("sib wait"):
        for e in (1, 3, 2, 0):
            q, dev = across(e)
            p = (y + e) % Y
            rcopy(s_acc.at[q], s_sib.at[p], sb_ss, sb_rs.at[p], sib, x).wait_recv()
            if e:
                s_send[p] = (s_acc[q] + s_sib[p]).astype(BF16)
                rcopy(s_send.at[p], s_recv.at[y], s_ss, s_rs.at[y], dev, x).start()

    def collect():
        for b in range(2):
            zb = 2 * x + b

            @pl.when(zb <= z)
            def _():
                with at("gwx wait"):
                    for side in range(2):
                        for h in range(2):
                            rcopy(
                                half(gw_send.at[zb], h), half(gwx.at[b, side], h),
                                gx_ss.at[zb], gx_rs.at[b, side, h], s, (x + 1 + 2 * side) % X,
                            ).wait_recv()
                gwr[b] = (
                    gw_send[zb].astype(F32) + gwx[b, 0].astype(F32) + gwx[b, 1].astype(F32)
                ).astype(BF16).reshape(R, T, T)
                for d in range(1, R):
                    q, dev = plane(d)
                    rcopy(
                        gwr.at[b, q], gwf.at[b, r], gf_ss.at[b], gf_rs.at[b], dev, x
                    ).start()
                gwf[b, r] = gwr[b, r]

            @pl.when(zb > z)
            def _():
                gwf[b] = jnp.zeros((R, T, T), BF16)

    lax.fori_loop(jnp.maximum(pairs - 2, 0), pairs, pass_pair, 0)

    @pl.when(z < 3)
    def _():
        collect()

    @pl.when(z < 6)
    def _():
        grad_normed()

    @pl.when(z >= 3)
    def _():
        collect()

    with at("red1 wait"):
        cp = rcopy(red1.at[1:], red1.at[1:], ra_ss, ra_rs, sib, x)
        cp.wait_recv()
        cp.wait_send()
    tot = red1[0]
    for q in range(1, R):
        tot = tot + red1[q]
    red2[z] = tot
    for d in range(1, Z):
        zz = (z + d) % Z
        rcopy(red2.at[z], red2.at[z], rb_ss, rb_rs, zz * R + r, x).start()
    acc = s_acc[r] + s_sib[y]
    with at("s wait"):
        for e in (1, 3, 2):
            p = (y + e) % Y
            q, dev = across(e)
            rcopy(s_send.at[p], s_recv.at[p], s_ss, s_rs.at[p], dev, x).wait_recv()
            acc = acc + s_recv[p].astype(F32)
    gg[...] = (go[...].astype(F32) * (acc + rows[1][:, 0:1])).astype(BF16)
    stores[0].start()

    with at("stat2 wait"):
        x_wait(stat2, sp_ss, sp_rs)
    tot = stat2[0] + stat2[1] + stat2[2] + stat2[3]
    colm = jnp.concatenate([tot, jnp.zeros((T - 8, T), F32)], axis=0).T
    centred = cen[...]
    gc = gn_own[...] * gain[...]
    gv[...] = (
        rows[0][:, 0:1] * (gc - colm[:, 0:1] / hidden - centred * (colm[:, 1:2] / hidden))
    ).astype(BF16)
    stores[2].start()


    for b in range(2):
        zb = 2 * x + b

        @pl.when(zb <= z)
        def _():
            with at("gwf wait"):
                cp = rcopy(gwr.at[b, 1:], gwf.at[b, 1:], gf_ss.at[b], gf_rs.at[b], sib, x)
                cp.wait_recv()
                cp.wait_send()

        for q in range(R):
            some = pl.ds((b * R + q) * T, T)
            pltpu.make_async_copy(gwf.at[b, q], gw_out.at[:, some], gw_sem).start()

    rcopy(s_send.at[1:], s_recv.at[1:], s_ss, s_rs.at[0], sib, x).wait_send()
    rcopy(g_all.at[1:], g_all.at[1:], g_ss, gb_rs, sib, x).wait_send()
    rcopy(s_sib, s_sib, sb_ss, sb_rs.at[0], sib, x).wait_send()

    def drain_w(k, carry):
        @pl.when(shared(k))
        def _():
            sent = wt.at[0, 1:, quarter]
            rcopy(sent, sent, w_ss.at[k], w_rs.at[0], sib, x).wait_send()

        @pl.when(jnp.logical_not(shared(k)))
        def _():
            sent = wt.at[0, 1:]
            rcopy(sent, sent, w_ss.at[k], w_rs.at[0], sib, x).wait_send()

        zz = k
        role = (x - zz // 2 + X) % X

        @pl.when(role == 2)
        def _():
            rcopy(gw_send.at[0], gw_send.at[0], go_ss.at[zz], go_rs.at[0], sib, x).wait_send()

        @pl.when(role % 2 == 1)
        def _():
            rcopy(gw_send.at[0], gw_send.at[0], gx_ss.at[zz], go_rs.at[0], sib, x).wait_send()

        return carry

    with at("drain"):
        lax.fori_loop(0, z + 1, drain_w, 0)

    def drain_gn(zz, carry):
        rcopy(
            gn_send.at[zz], gn_recv.at[z], gn_ss.at[zz], gn_rs.at[z], zz * R + r, x
        ).wait_send()
        return carry

    lax.fori_loop(0, z, drain_gn, 0)

    for d in range(1, Z):

        @pl.when(z + d < Z)
        def _():
            rcopy(n_all.at[z], n_all.at[z], n_ss.at[z + d], n_rs.at[z], sib, x).wait_send()

    with at("red2 wait"):
        cp = rcopy(red2.at[1:], red2.at[1:], rb_ss, rb_rs, sib, x)
        cp.wait_recv()
        cp.wait_send()
    tot = red2[0]
    for q in range(1, Z):
        tot = tot + red2[q]
    gs[...] = tot
    stores[3].start()
    with at("store wait"):
        for store in stores:
            store.wait()
        pltpu.make_async_copy(gwf, gwf, gw_sem).wait()


def finish(
    gg_in, gv_in, gs_in, gw_in, tb_in, gg_out, gv_out, gain_out, shift_out, gw_out, tb_out,
    gg, gv, gs, gw, tb, gw_f, in_sem, sem,
):
    rows, width = gw_f.shape
    loads = [
        pltpu.make_async_copy(a, b, in_sem.at[i])
        for i, (a, b) in enumerate(
            ((gw_in, gw), (gg_in, gg), (gv_in, gv), (gs_in, gs), (tb_in, tb))
        )
    ]
    for load in loads:
        load.start()
    row = lax.axis_index("seq") * rows + lax.broadcasted_iota(jnp.int32, (rows, T), 0)
    lane = lax.axis_index("hid") * width + lax.broadcasted_iota(jnp.int32, (rows, T), 1)
    loads[0].wait()
    copies = []
    for q in range(width // T):
        cols = slice(q * T, (q + 1) * T)
        gw_f[:, cols] = jnp.where(lane + q * T <= row, gw[:, cols].astype(F32), 0.0)
        if q % 4 == 3:
            some = pl.ds((q - 3) * T, 4 * T)
            copies.append(
                pltpu.make_async_copy(gw_f.at[:, some], gw_out.at[:, some], sem.at[5 + q // 4])
            )
            copies[-1].start()
        if q == 3:
            for load in loads[1:]:
                load.wait()
            for i, (a, b) in enumerate((
                (gg, gg_out), (gv, gv_out), (tb, tb_out),
                (gs.at[0:1], gain_out), (gs.at[1:2], shift_out),
            )):
                copies.append(pltpu.make_async_copy(a, b, sem.at[i]))
                copies[-1].start()
    for copy in copies:
        copy.wait()


def per_device(gate_half, value_half, norm_gain, norm_shift, token_weight, token_bias, grad_output):
    rows, chans = gate_half.shape
    cols = token_weight.shape[1]
    width = cols // X
    dma = pltpu.SemaphoreType.DMA
    anywhere = pl.BlockSpec(memory_space=pl.ANY)
    gg, gv, gs, gw, tb = pl.pallas_call(
        functools.partial(kernel, chans * X),
        out_shape=(
            jax.ShapeDtypeStruct((rows, chans), BF16),
            jax.ShapeDtypeStruct((rows, chans), BF16),
            jax.ShapeDtypeStruct((2, chans), F32),
            jax.ShapeDtypeStruct((rows, width), BF16),
            jax.ShapeDtypeStruct((1, rows), F32),
        ),
        in_specs=[anywhere] * 7,
        out_specs=(anywhere,) * 5,
        scratch_shapes=[
            pltpu.VMEM((R, T, chans), BF16),
            pltpu.VMEM((Z, T, chans), BF16),
            pltpu.VMEM((Z, R, T, T), BF16),
            pltpu.VMEM((R, T, chans), F32),
            pltpu.VMEM((Y, T, chans), F32),
            pltpu.VMEM((Y, T, chans), BF16),
            pltpu.VMEM((Y, T, chans), BF16),
            pltpu.VMEM((T, chans), F32),
            pltpu.VMEM((Z, T, chans), BF16),
            pltpu.VMEM((Z, T, chans), BF16),
            pltpu.VMEM((Z, R * T, T), BF16),
            pltpu.VMEM((Z, R * T // 2, T), BF16),
            pltpu.VMEM((2, 2, R * T, T), BF16),
            pltpu.VMEM((2, R, T, T), BF16),
            pltpu.VMEM((2, R, T, T), BF16),
            pltpu.VMEM((X, 8, T), F32),
            pltpu.VMEM((X, 8, T), F32),
            pltpu.VMEM((R, 2, chans), F32),
            pltpu.VMEM((Z, 2, chans), F32),
            pltpu.VMEM((T, chans), F32),
            pltpu.VMEM((2, T, T), F32),
            pltpu.VMEM((rows, chans), BF16),
            pltpu.VMEM((rows, chans), BF16),
            pltpu.VMEM((1, chans), F32),
            pltpu.VMEM((1, chans), F32),
            pltpu.VMEM((rows, cols), BF16),
            pltpu.VMEM((1, rows), F32),
            pltpu.VMEM((rows, chans), BF16),
            dma((7,)),
            pltpu.VMEM((rows, chans), BF16),
            pltpu.VMEM((rows, chans), BF16),
            pltpu.VMEM((2, chans), F32),
            pltpu.VMEM((1, rows), F32),
            dma((4,)), dma(()),
            dma(()), dma((R,)), dma(()),
            dma((Z,)), dma((Z,)),
            dma((Z,)), dma((Z,)),
            dma((Z,)), dma((Z,)),
            dma(()), dma((Y,)),
            dma(()), dma((Y,)),
            dma((Z,)), dma((Z,)),
            dma((Z,)), dma((Z,)),
            dma((Z,)), dma((2, 2, 2)),
            dma((2,)), dma((2,)),
            *([dma(())] * 8),
        ],
        compiler_params=pltpu.CompilerParams(
            collective_id=0, has_side_effects=True, vmem_limit_bytes=60 * 1024 * 1024
        ),
    )(
        gate_half, value_half, norm_gain[None], norm_shift[None], token_weight, token_bias[None],
        grad_output,
    )
    gg, gv, gain, shift, gw, tb = pl.pallas_call(
        finish,
        out_shape=(
            jax.ShapeDtypeStruct((rows, chans), BF16),
            jax.ShapeDtypeStruct((rows, chans), BF16),
            jax.ShapeDtypeStruct((1, chans), F32),
            jax.ShapeDtypeStruct((1, chans), F32),
            jax.ShapeDtypeStruct((rows, width), F32),
            jax.ShapeDtypeStruct((1, rows), F32),
        ),
        in_specs=[anywhere] * 5,
        out_specs=(anywhere,) * 6,
        scratch_shapes=[
            pltpu.VMEM((rows, chans), BF16),
            pltpu.VMEM((rows, chans), BF16),
            pltpu.VMEM((2, chans), F32),
            pltpu.VMEM((rows, width), BF16),
            pltpu.VMEM((1, rows), F32),
            pltpu.VMEM((rows, width), F32),
            dma((5,)),
            dma((5 + width // T // 4,)),
        ],
        compiler_params=pltpu.CompilerParams(vmem_limit_bytes=60 * 1024 * 1024),
    )(gg, gv, gs, gw, tb)
    return gg, gv, gain[0], shift[0], gw, tb[0]


def solution(mesh):
    placed = (
        P("seq", "hid"),
        P("seq", "hid"),
        P("hid"),
        P("hid"),
        P("seq", None),
        P("seq"),
        P("seq", "hid"),
    )
    return jax.shard_map(
        per_device,
        mesh=mesh,
        in_specs=placed,
        out_specs=(P("seq", "hid"), P("seq", "hid"), P("hid"), P("hid"), P("seq", "hid"), P("seq")),
        check_vma=False,
    )
```

```python
import contextlib
import functools

import jax
import jax.numpy as jnp
from jax import lax
from jax.experimental import pallas as pl
from jax.experimental.pallas import tpu as pltpu
from jax.sharding import PartitionSpec as P

MESH = pl.DeviceIdType.MESH
F32 = jnp.float32
BF16 = jnp.bfloat16
T = 128
R = 8
Z = 8
X = 4
Y = 4


def at(name):
    return contextlib.nullcontext()


def dot(a, b, ca, cb):
    return lax.dot_general(a, b, (((ca,), (cb,)), ((), ())), preferred_element_type=F32)


def kernel(
    hidden,
    gate_h, value_h, gain_h, shift_h, w_h, tbias_h, go_h,
    gg_out, gv_out, gs_out, gw_out, tb_out,
    g_all, n_all, wt, s_acc, s_sib, s_send, s_recv, gn_own, gn_send, gn_recv,
    gw_send, gwo, gwx, gwr, gwf,
    stat1, stat2, red1, red2, cen, rows,
    gate, value, gain, shift, w, tbias, go, in_sem,
    gg, gv, gs, tb, out_sem, gw_sem,
    g_ss, g_rs, gb_rs, w_ss, w_rs, f_ss, f_rs, n_ss, n_rs, sb_ss, sb_rs, s_ss, s_rs, gn_ss, gn_rs,
    go_ss, go_rs, gx_ss, gx_rs, gf_ss, gf_rs,
    st_ss, st_rs, sp_ss, sp_rs, ra_ss, ra_rs, rb_ss, rb_rs,
):
    s = lax.axis_index("seq")
    x = lax.axis_index("hid")
    z = s // R
    r = s % R
    y = r // 2
    c = r % 2
    sib = z * R + y * 2 + (1 - c)
    H = R * T // 2

    def rcopy(src, dst, ss, rs, ds, dx):
        return pltpu.make_async_remote_copy(
            src_ref=src, dst_ref=dst, send_sem=ss, recv_sem=rs,
            device_id=(ds, dx), device_id_type=MESH,
        )

    def plane(d):
        q = (r + d) % R
        return q, z * R + q

    def across(e):
        q = (y + e) % Y * 2 + c
        return q, z * R + q

    def chunk(k, core):
        p = (k + core * ((z + 1) // 2)) % (z + 1)
        evens = (z + 2) // 2
        p = z - jnp.where(p < evens, 2 * p, 2 * (p - evens) + 1)
        return jnp.where(k > z, z + 1, p)

    def first(k):
        return jnp.where(k > z, z + 1, jnp.where((k < 4) & (z >= 4), (k + z) % 4, k))

    n_shared = jnp.maximum(z - Z // 2, 0)
    quarter = pl.ds(pl.multiple_of(x * (T // X), T // X), T // X)

    def shared(k):
        return (k % 2 == 0) & (k < 2 * n_shared)

    def columns(zz, q):
        return pl.ds(pl.multiple_of((zz * R + q) * T, T), T)

    def share_send(m, carry):
        for d in range(1, R):
            q, dev = plane(d)
            zz = first(2 * m)
            rcopy(
                w.at[quarter, columns(zz, q)], wt.at[zz, r, quarter],
                w_ss.at[2 * m], w_rs.at[zz], dev, x,
            ).start()
        zz = first(2 * m)
        wt[zz, r, quarter] = w[quarter, columns(zz, r)]
        return carry

    def share_pass(m, carry):
        zz = first(2 * m)
        got = wt.at[zz, 1:, quarter]
        rcopy(got, got, w_ss.at[zz], w_rs.at[zz], sib, x).wait_recv()
        for d in range(1, X):
            t = (x + d) % X
            part = wt.at[zz, :, quarter]
            rcopy(part, part, f_ss.at[zz], f_rs.at[zz], s, t).start()
        return carry

    loads = [
        pltpu.make_async_copy(a, b, in_sem.at[i])
        for i, (a, b) in enumerate((
            (value_h, value), (go_h, go), (gate_h, gate), (w_h, w),
            (gain_h, gain), (shift_h, shift), (tbias_h, tbias),
        ))
    ]
    for load in loads:
        load.start()

    barrier = pltpu.get_barrier_semaphore()
    for d in range(1, R):
        q, dev = plane(d)
        pl.semaphore_signal(barrier, inc=1, device_id=(dev, x), device_id_type=MESH)
    for d in range(1, Z):
        pl.semaphore_signal(
            barrier, inc=1, device_id=((z + d) % Z * R + r, x), device_id_type=MESH
        )
    for d in range(1, X):
        pl.semaphore_signal(barrier, inc=1, device_id=(s, (x + d) % X), device_id_type=MESH)

    for load in loads[:3]:
        load.wait()
    v = value[...].astype(F32)
    gm = (go[...].astype(F32) * gate[...].astype(F32)).astype(BF16)
    g_all[r] = gm
    lane = lax.broadcasted_iota(jnp.int32, (T, T), 1)

    def as_rows(cols):
        m = jnp.zeros((T, T), F32)
        for i, col in enumerate(cols):
            m = jnp.where(lane == i, col, m)
        return m.T[:8]

    stat1[x] = as_rows((
        jnp.sum(v, axis=1, keepdims=True),
        jnp.sum(v * v, axis=1, keepdims=True),
        jnp.sum(gm.astype(F32), axis=1, keepdims=True),
    ))
    for load in loads[3:]:
        load.wait()
    with at("barrier"):
        pl.semaphore_wait(barrier, (R - 1) + (Z - 1) + (X - 1))

    def x_send(buf, ss, rs):
        for d in range(1, X):
            t = (x + d) % X
            rcopy(buf.at[x], buf.at[x], ss, rs, s, t).start()

    def x_wait(buf, ss, rs):
        cp = rcopy(buf.at[1:], buf.at[1:], ss, rs, sib, x)
        cp.wait_recv()
        cp.wait_send()

    x_send(stat1, st_ss, st_rs)
    lax.fori_loop(0, n_shared, share_send, 0)
    for e in (1, 3, 2):
        q, dev = across(e)
        rcopy(g_all.at[r], g_all.at[r], g_ss, g_rs.at[r], dev, x).start()
    rcopy(g_all.at[r], g_all.at[r], g_ss, gb_rs, sib, x).start()

    def w_send(k, carry):
        @pl.when(jnp.logical_not(shared(k)))
        def _():
            for d in range(1, R):
                q, dev = plane(d)
                zz = first(k)
                rcopy(
                    w.at[:, columns(zz, q)], wt.at[zz, r], w_ss.at[k], w_rs.at[zz], dev, x
                ).start()

        return carry

    with at("w send"):
        lax.fori_loop(0, z + 1, w_send, 0)

    with at("stat wait"):
        x_wait(stat1, st_ss, st_rs)
    tot = stat1[0] + stat1[1] + stat1[2] + stat1[3]
    tb[...] = tot[2:3]
    colm = jnp.concatenate([tot[:3], tbias[...], jnp.zeros((T - 4, T), F32)], axis=0).T
    mean = colm[:, 0:1] / hidden
    var = colm[:, 1:2] / hidden - mean * mean
    inv = lax.rsqrt(var + 1e-05)
    centred = (v - mean) * inv
    cen[...] = centred
    rows[0] = jnp.broadcast_to(inv, (T, T))
    rows[1] = jnp.broadcast_to(colm[:, 3:4], (T, T))
    n_all[z] = (centred * gain[...] + shift[...]).astype(BF16)

    with at("n send"):
        for d in (1, 7, 2, 6, 3, 5, 4):
            zz = z + d

            @pl.when(zz < Z)
            def _():
                rcopy(n_all.at[z], n_all.at[z], n_ss.at[zz], n_rs.at[z], zz * R + r, x).start()

    with at("share pass"):
        lax.fori_loop(0, n_shared, share_pass, 0)

    with at("g wait"):
        for e in (1, 3, 2):
            q, dev = across(e)
            rcopy(g_all.at[q], g_all.at[q], g_ss, g_rs.at[q], dev, x).wait_recv()
            rcopy(g_all.at[q], g_all.at[q], g_ss, gb_rs, sib, x).start()
        rcopy(g_all.at[Y:], g_all.at[Y:], g_ss, gb_rs, sib, x).wait_recv()

    def arrive(k):
        zz = first(k)

        @pl.when(shared(k))
        def _():
            with at("share wait"):
                got = wt.at[zz, :, : T - T // X]
                cp = rcopy(got, got, f_ss.at[zz], f_rs.at[zz], sib, x)
                cp.wait_recv()
                cp.wait_send()

        @pl.when(jnp.logical_not(shared(k)) & (k <= z))
        def _():
            with at("w wait"):
                got = wt.at[zz, 1:]
                rcopy(got, got, w_ss.at[zz], w_rs.at[zz], sib, x).wait_recv()
            wt[zz, r] = w[:, columns(zz, r)]

        @pl.when(zz == z)
        def _():
            row = lax.broadcasted_iota(jnp.int32, (T, T), 0)
            own = wt[zz, r].astype(F32)
            wt[zz, r] = jnp.where(row >= lane, own, 0.0).astype(BF16)

            def clear(q, carry):
                wt[zz, q] = jnp.zeros((T, T), BF16)
                return carry

            lax.fori_loop(0, r, clear, 0)

        return zz

    def both(a, b):
        return jnp.concatenate([wt[a].reshape(R * T, T), wt[b].reshape(R * T, T)], axis=1)

    def grad_part(p):
        pair = arrive(2 * p), arrive(2 * p + 1)
        gn = dot(both(*pair), g_all[...].reshape(R * T, -1), 0, 0)
        for i, zz in enumerate(pair):
            part = gn[i * T : (i + 1) * T]

            @pl.when(zz == z)
            def _():
                gn_own[...] = part

            far = z - zz

            @pl.when(far > 0)
            def _():
                gn_send[zz] = part.astype(BF16)

            @pl.when(far >= 1)
            def _():
                rcopy(
                    gn_send.at[zz], gn_recv.at[z], gn_ss.at[zz], gn_rs.at[z], zz * R + r, x
                ).start()

    def half(ref, h):
        return ref.at[pl.ds(pl.multiple_of(h * H, H), H), :]

    def norm_part(p):
        pair = chunk(2 * p, c), chunk(2 * p + 1, c)

        for zz in pair:

            @pl.when(zz < z)
            def _():
                with at("n wait"):
                    rcopy(
                        n_all.at[zz], n_all.at[zz], n_ss.at[zz], n_rs.at[zz], zz * R + r, x
                    ).wait_recv()

        nz = jnp.concatenate([n_all[pair[0]], n_all[pair[1]]], axis=0)
        prod = dot(g_all[...].reshape(R * T, -1), nz, 1, 1).astype(BF16)
        for i, zz in enumerate(pair):
            gw_send[zz] = prod[:, i * T : (i + 1) * T]
            t = zz // 2
            role = (x - t + X) % X

            @pl.when((role == 2) & (zz <= z))
            def _():
                for h, e in ((0, 1), (1, 3)):
                    rcopy(
                        half(gw_send.at[zz], h), gwo.at[zz], go_ss.at[zz], go_rs.at[zz],
                        s, (t + e) % X,
                    ).start()

            @pl.when((role % 2 == 1) & (zz <= z))
            def _():
                side = role // 2
                h = 1 - side
                rcopy(
                    half(gw_send.at[zz], h), half(gwx.at[zz % 2, side], h),
                    gx_ss.at[zz], gx_rs.at[zz % 2, side, h], s, t,
                ).start()

    def mix(p, carry):
        pair = 2 * p, 2 * p + 1
        nz = jnp.concatenate([n_all[pair[0]], n_all[pair[1]]], axis=0)
        sp = dot(both(*pair), nz, 1, 0).reshape(R, T, -1)

        @pl.when(p == 0)
        def _():
            s_acc[...] = sp

        @pl.when(p > 0)
        def _():
            s_acc[...] += sp

        return carry

    def pass_part(j):
        zz = chunk(j, c)
        t = zz // 2
        role = (x - t + X) % X

        @pl.when((role % 2 == 1) & (zz <= z))
        def _():
            side = role // 2
            with at("gwo wait"):
                rcopy(gwo.at[zz], gwo.at[zz], go_ss.at[zz], go_rs.at[zz], s, t).wait_recv()
            mine = half(gw_send.at[zz], side)
            mine[...] = (mine[...].astype(F32) + gwo[zz].astype(F32)).astype(BF16)
            rcopy(
                mine, half(gwx.at[zz % 2, side], side),
                gx_ss.at[zz], gx_rs.at[zz % 2, side, side], s, t,
            ).start()

    @pl.when(z % 2 == 0)
    def _():
        wt[z + 1] = jnp.zeros((R, T, T), BF16)
        n_all[z + 1] = jnp.zeros((T, n_all.shape[2]), BF16)

    pairs = (z + 2) // 2
    lag = jnp.where(z == Z - 1, 1, 2)

    def step(k, carry):
        @pl.when(k < pairs)
        def _():
            grad_part(k)

        @pl.when((k >= lag) & (k < pairs + lag))
        def _():
            norm_part(k - lag)

        @pl.when((k >= lag + 2) & (z == Z - 1))
        def _():
            pass_pair(k - lag - 2, 0)

        return carry

    def pass_pair(p, carry):
        pass_part(2 * p)
        pass_part(2 * p + 1)
        return carry

    lax.fori_loop(0, pairs + lag, step, 0)
    lax.fori_loop(0, pairs, mix, 0)

    stores = [
        pltpu.make_async_copy(a, b, out_sem.at[i])
        for i, (a, b) in enumerate(((gg, gg_out), (tb, tb_out), (gv, gv_out), (gs, gs_out)))
    ]
    stores[1].start()

    for e in range(Y):
        q = (y + e) % Y
        rcopy(s_acc.at[q * 2 + 1 - c], s_sib.at[q], sb_ss, sb_rs.at[q], sib, x).start()
    def grad_normed():
        with at("gn wait"):
            for d in range(1, Z):
                zz = z + d

                @pl.when(zz < Z)
                def _():
                    rcopy(
                        gn_send.at[0], gn_recv.at[zz], gn_ss.at[0], gn_rs.at[zz], sib, x
                    ).wait_recv()
                    gn_own[...] += gn_recv[zz].astype(F32)

        gn = gn_own[...]
        centred = cen[...]
        gc = gn * gain[...]
        stat2[x] = as_rows((
            jnp.sum(gc, axis=1, keepdims=True),
            jnp.sum(gc * centred, axis=1, keepdims=True),
        ))
        x_send(stat2, sp_ss, sp_rs)
        red1[r] = jnp.concatenate([
            jnp.sum(gn * centred, axis=0, keepdims=True),
            jnp.sum(gn, axis=0, keepdims=True),
        ], axis=0)
        for d in range(1, R):
            q, dev = plane(d)
            rcopy(red1.at[r], red1.at[r], ra_ss, ra_rs, dev, x).start()
    @pl.when(z == Z - 1)
    def _():
        grad_normed()

    with at("sib wait"):
        for e in (1, 3, 2, 0):
            q, dev = across(e)
            p = (y + e) % Y
            rcopy(s_acc.at[q], s_sib.at[p], sb_ss, sb_rs.at[p], sib, x).wait_recv()
            if e:
                s_send[p] = (s_acc[q] + s_sib[p]).astype(BF16)
                rcopy(s_send.at[p], s_recv.at[y], s_ss, s_rs.at[y], dev, x).start()

    def collect():
        for b in range(2):
            zb = 2 * x + b

            @pl.when(zb <= z)
            def _():
                with at("gwx wait"):
                    for side in range(2):
                        for h in range(2):
                            rcopy(
                                half(gw_send.at[zb], h), half(gwx.at[b, side], h),
                                gx_ss.at[zb], gx_rs.at[b, side, h], s, (x + 1 + 2 * side) % X,
                            ).wait_recv()
                gwr[b] = (
                    gw_send[zb].astype(F32) + gwx[b, 0].astype(F32) + gwx[b, 1].astype(F32)
                ).astype(BF16).reshape(R, T, T)
                for d in range(1, R):
                    q, dev = plane(d)
                    rcopy(
                        gwr.at[b, q], gwf.at[b, r], gf_ss.at[b], gf_rs.at[b], dev, x
                    ).start()
                gwf[b, r] = gwr[b, r]

            @pl.when(zb > z)
            def _():
                gwf[b] = jnp.zeros((R, T, T), BF16)

    lax.fori_loop(jnp.where(z == Z - 1, pairs - 2, 0), pairs, pass_pair, 0)

    @pl.when(z < 3)
    def _():
        collect()

    @pl.when(z < Z - 1)
    def _():
        grad_normed()

    with at("red1 wait"):
        cp = rcopy(red1.at[1:], red1.at[1:], ra_ss, ra_rs, sib, x)
        cp.wait_recv()
        cp.wait_send()
    tot = red1[0]
    for q in range(1, R):
        tot = tot + red1[q]
    red2[z] = tot
    for d in range(1, Z):
        zz = (z + d) % Z
        rcopy(red2.at[z], red2.at[z], rb_ss, rb_rs, zz * R + r, x).start()
    @pl.when(z >= 3)
    def _():
        collect()

    acc = s_acc[r] + s_sib[y]
    with at("s wait"):
        for e in (1, 3, 2):
            p = (y + e) % Y
            q, dev = across(e)
            rcopy(s_send.at[p], s_recv.at[p], s_ss, s_rs.at[p], dev, x).wait_recv()
            acc = acc + s_recv[p].astype(F32)
    gg[...] = (go[...].astype(F32) * (acc + rows[1][:, 0:1])).astype(BF16)
    stores[0].start()

    with at("stat2 wait"):
        x_wait(stat2, sp_ss, sp_rs)
    tot = stat2[0] + stat2[1] + stat2[2] + stat2[3]
    colm = jnp.concatenate([tot, jnp.zeros((T - 8, T), F32)], axis=0).T
    centred = cen[...]
    gc = gn_own[...] * gain[...]
    gv[...] = (
        rows[0][:, 0:1] * (gc - colm[:, 0:1] / hidden - centred * (colm[:, 1:2] / hidden))
    ).astype(BF16)
    stores[2].start()


    for b in range(2):
        zb = 2 * x + b

        @pl.when(zb <= z)
        def _():
            with at("gwf wait"):
                cp = rcopy(gwr.at[b, 1:], gwf.at[b, 1:], gf_ss.at[b], gf_rs.at[b], sib, x)
                cp.wait_recv()
                cp.wait_send()

        for q in range(R):
            some = pl.ds((b * R + q) * T, T)
            pltpu.make_async_copy(gwf.at[b, q], gw_out.at[:, some], gw_sem).start()

    rcopy(s_send.at[1:], s_recv.at[1:], s_ss, s_rs.at[0], sib, x).wait_send()
    rcopy(g_all.at[1:], g_all.at[1:], g_ss, gb_rs, sib, x).wait_send()
    rcopy(s_sib, s_sib, sb_ss, sb_rs.at[0], sib, x).wait_send()

    def drain_w(k, carry):
        @pl.when(shared(k))
        def _():
            sent = wt.at[0, 1:, quarter]
            rcopy(sent, sent, w_ss.at[k], w_rs.at[0], sib, x).wait_send()

        @pl.when(jnp.logical_not(shared(k)))
        def _():
            sent = wt.at[0, 1:]
            rcopy(sent, sent, w_ss.at[k], w_rs.at[0], sib, x).wait_send()

        zz = k
        role = (x - zz // 2 + X) % X

        @pl.when(role == 2)
        def _():
            rcopy(gw_send.at[0], gw_send.at[0], go_ss.at[zz], go_rs.at[0], sib, x).wait_send()

        @pl.when(role % 2 == 1)
        def _():
            rcopy(gw_send.at[0], gw_send.at[0], gx_ss.at[zz], go_rs.at[0], sib, x).wait_send()

        return carry

    with at("drain"):
        lax.fori_loop(0, z + 1, drain_w, 0)

    def drain_gn(zz, carry):
        rcopy(
            gn_send.at[zz], gn_recv.at[z], gn_ss.at[zz], gn_rs.at[z], zz * R + r, x
        ).wait_send()
        return carry

    lax.fori_loop(0, z, drain_gn, 0)

    for d in range(1, Z):

        @pl.when(z + d < Z)
        def _():
            rcopy(n_all.at[z], n_all.at[z], n_ss.at[z + d], n_rs.at[z], sib, x).wait_send()

    with at("red2 wait"):
        cp = rcopy(red2.at[1:], red2.at[1:], rb_ss, rb_rs, sib, x)
        cp.wait_recv()
        cp.wait_send()
    tot = red2[0]
    for q in range(1, Z):
        tot = tot + red2[q]
    gs[...] = tot
    stores[3].start()
    with at("store wait"):
        for store in stores:
            store.wait()
        pltpu.make_async_copy(gwf, gwf, gw_sem).wait()


def finish(
    gg_in, gv_in, gs_in, gw_in, tb_in, gg_out, gv_out, gain_out, shift_out, gw_out, tb_out,
    gg, gv, gs, gw, tb, gw_f, in_sem, sem,
):
    rows, width = gw_f.shape
    loads = [
        pltpu.make_async_copy(a, b, in_sem.at[i])
        for i, (a, b) in enumerate(
            ((gw_in, gw), (gg_in, gg), (gv_in, gv), (gs_in, gs), (tb_in, tb))
        )
    ]
    for load in loads:
        load.start()
    row = lax.axis_index("seq") * rows + lax.broadcasted_iota(jnp.int32, (rows, T), 0)
    lane = lax.axis_index("hid") * width + lax.broadcasted_iota(jnp.int32, (rows, T), 1)
    loads[0].wait()
    copies = []
    for q in range(width // T):
        cols = slice(q * T, (q + 1) * T)
        gw_f[:, cols] = jnp.where(lane + q * T <= row, gw[:, cols].astype(F32), 0.0)
        if q % 4 == 3:
            some = pl.ds((q - 3) * T, 4 * T)
            copies.append(
                pltpu.make_async_copy(gw_f.at[:, some], gw_out.at[:, some], sem.at[5 + q // 4])
            )
            copies[-1].start()
        if q == 3:
            for load in loads[1:]:
                load.wait()
            for i, (a, b) in enumerate((
                (gg, gg_out), (gv, gv_out), (tb, tb_out),
                (gs.at[0:1], gain_out), (gs.at[1:2], shift_out),
            )):
                copies.append(pltpu.make_async_copy(a, b, sem.at[i]))
                copies[-1].start()
    for copy in copies:
        copy.wait()


def per_device(gate_half, value_half, norm_gain, norm_shift, token_weight, token_bias, grad_output):
    rows, chans = gate_half.shape
    cols = token_weight.shape[1]
    width = cols // X
    dma = pltpu.SemaphoreType.DMA
    anywhere = pl.BlockSpec(memory_space=pl.ANY)
    gg, gv, gs, gw, tb = pl.pallas_call(
        functools.partial(kernel, chans * X),
        out_shape=(
            jax.ShapeDtypeStruct((rows, chans), BF16),
            jax.ShapeDtypeStruct((rows, chans), BF16),
            jax.ShapeDtypeStruct((2, chans), F32),
            jax.ShapeDtypeStruct((rows, width), BF16),
            jax.ShapeDtypeStruct((1, rows), F32),
        ),
        in_specs=[anywhere] * 7,
        out_specs=(anywhere,) * 5,
        scratch_shapes=[
            pltpu.VMEM((R, T, chans), BF16),
            pltpu.VMEM((Z, T, chans), BF16),
            pltpu.VMEM((Z, R, T, T), BF16),
            pltpu.VMEM((R, T, chans), F32),
            pltpu.VMEM((Y, T, chans), F32),
            pltpu.VMEM((Y, T, chans), BF16),
            pltpu.VMEM((Y, T, chans), BF16),
            pltpu.VMEM((T, chans), F32),
            pltpu.VMEM((Z, T, chans), BF16),
            pltpu.VMEM((Z, T, chans), BF16),
            pltpu.VMEM((Z, R * T, T), BF16),
            pltpu.VMEM((Z, R * T // 2, T), BF16),
            pltpu.VMEM((2, 2, R * T, T), BF16),
            pltpu.VMEM((2, R, T, T), BF16),
            pltpu.VMEM((2, R, T, T), BF16),
            pltpu.VMEM((X, 8, T), F32),
            pltpu.VMEM((X, 8, T), F32),
            pltpu.VMEM((R, 2, chans), F32),
            pltpu.VMEM((Z, 2, chans), F32),
            pltpu.VMEM((T, chans), F32),
            pltpu.VMEM((2, T, T), F32),
            pltpu.VMEM((rows, chans), BF16),
            pltpu.VMEM((rows, chans), BF16),
            pltpu.VMEM((1, chans), F32),
            pltpu.VMEM((1, chans), F32),
            pltpu.VMEM((rows, cols), BF16),
            pltpu.VMEM((1, rows), F32),
            pltpu.VMEM((rows, chans), BF16),
            dma((7,)),
            pltpu.VMEM((rows, chans), BF16),
            pltpu.VMEM((rows, chans), BF16),
            pltpu.VMEM((2, chans), F32),
            pltpu.VMEM((1, rows), F32),
            dma((4,)), dma(()),
            dma(()), dma((R,)), dma(()),
            dma((Z,)), dma((Z,)),
            dma((Z,)), dma((Z,)),
            dma((Z,)), dma((Z,)),
            dma(()), dma((Y,)),
            dma(()), dma((Y,)),
            dma((Z,)), dma((Z,)),
            dma((Z,)), dma((Z,)),
            dma((Z,)), dma((2, 2, 2)),
            dma((2,)), dma((2,)),
            *([dma(())] * 8),
        ],
        compiler_params=pltpu.CompilerParams(
            collective_id=0, has_side_effects=True, vmem_limit_bytes=60 * 1024 * 1024
        ),
    )(
        gate_half, value_half, norm_gain[None], norm_shift[None], token_weight, token_bias[None],
        grad_output,
    )
    gg, gv, gain, shift, gw, tb = pl.pallas_call(
        finish,
        out_shape=(
            jax.ShapeDtypeStruct((rows, chans), BF16),
            jax.ShapeDtypeStruct((rows, chans), BF16),
            jax.ShapeDtypeStruct((1, chans), F32),
            jax.ShapeDtypeStruct((1, chans), F32),
            jax.ShapeDtypeStruct((rows, width), F32),
            jax.ShapeDtypeStruct((1, rows), F32),
        ),
        in_specs=[anywhere] * 5,
        out_specs=(anywhere,) * 6,
        scratch_shapes=[
            pltpu.VMEM((rows, chans), BF16),
            pltpu.VMEM((rows, chans), BF16),
            pltpu.VMEM((2, chans), F32),
            pltpu.VMEM((rows, width), BF16),
            pltpu.VMEM((1, rows), F32),
            pltpu.VMEM((rows, width), F32),
            dma((5,)),
            dma((5 + width // T // 4,)),
        ],
        compiler_params=pltpu.CompilerParams(vmem_limit_bytes=60 * 1024 * 1024),
    )(gg, gv, gs, gw, tb)
    return gg, gv, gain[0], shift[0], gw, tb[0]


def solution(mesh):
    placed = (
        P("seq", "hid"),
        P("seq", "hid"),
        P("hid"),
        P("hid"),
        P("seq", None),
        P("seq"),
        P("seq", "hid"),
    )
    return jax.shard_map(
        per_device,
        mesh=mesh,
        in_specs=placed,
        out_specs=(P("seq", "hid"), P("seq", "hid"), P("hid"), P("hid"), P("seq", "hid"), P("seq")),
        check_vma=False,
    )
```
